32 devices in a mesh: dp: 4 (over y, core), seq: 4 (over z), head: 2 (over x).
Axes of the slice: x: 2, y: 2, z: 4, core: 2. Of those that a mesh axis runs over, the one named last changes fastest.
Arguments:
- tokens: bfloat16 [8, 2048, 1536], P('dp', 'seq'), may hold values from -6 to 6
- cotangent: bfloat16 [8, 2048, 1536], P('dp', 'seq'), may hold values from -6 to 6
- doc_start: int32 [8, 2048], P('dp', 'seq'), may hold values from 0 to 2047, as said below
- norm_gain: float32 [1536], replicated, may hold values from 0.5 to 1.5
- gate_proj: bfloat16 [1536, 3072], P('seq', 'head'), may hold values from -0.15625 to 0.15625
- input_proj: bfloat16 [1536, 3072], P('seq', 'head'), may hold values from -0.15625 to 0.15625
- state_proj: bfloat16 [1536, 256], P('seq'), may hold values from -0.15625 to 0.15625
- step_proj: bfloat16 [1536, 48], P('seq', 'head'), may hold values from -0.15625 to 0.15625
- inner_kernel: float32 [4, 3072], P(None, 'head'), may hold values from -3 to 3
- inner_shift: float32 [3072], P('head'), may hold values from -3 to 3
- state_kernel: float32 [4, 256], replicated, may hold values from -3 to 3
- state_shift: float32 [256], replicated, may hold values from -3 to 3
- step_bias: float32 [48], P('head'), may hold values from -4 to -1
- decay_log: float32 [48], P('head'), may hold values from -9 to 0.5
- skip_gain: float32 [48], P('head'), may hold values from 0.5 to 2
- inner_gain: float32 [3072], P('head'), may hold values from 0.5 to 1.5
- out_proj: bfloat16 [3072, 1536], P('head', 'seq'), may hold values from -0.109375 to 0.109375
Outputs:
- block_out: bfloat16 [8, 2048, 1536], P('dp', 'seq')
- grad_tokens: bfloat16 [8, 2048, 1536], P('dp', 'seq')
- grad_norm_gain: float32 [1536], replicated
- grad_gate_proj: float32 [1536, 3072], P('seq', 'head')
- grad_input_proj: float32 [1536, 3072], P('seq', 'head')
- grad_state_proj: float32 [1536, 256], P('seq')
- grad_step_proj: float32 [1536, 48], P('seq', 'head')
- grad_inner_kernel: float32 [4, 3072], P(None, 'head')
- grad_inner_shift: float32 [3072], P('head')
- grad_state_kernel: float32 [4, 256], replicated
- grad_state_shift: float32 [256], replicated
- grad_step_bias: float32 [48], P('head')
- grad_decay_log: float32 [48], P('head')
- grad_skip_gain: float32 [48], P('head')
- grad_inner_gain: float32 [3072], P('head')
- grad_out_proj: float32 [3072, 1536], P('head', 'seq')
The draws below stay inside these ranges and needn't reach their ends.
Inputs may be any that keep to these rules, and one draw needn't show every extreme that they name: doc_start[s, t] is the position within sequence s of the first token of the document that holds token t: 0 for t = 0, never falling along t, at most t; every document that another follows has 200 to 2000 tokens, except that in the last sequence the final token forms a document of its own and the one before it may be shorter.
All inputs are finite; a program needn't handle non-finite values.
Results may differ from the reference program's by a relative error of at most 0.012.
The reference program's roundings to bfloat16 on the way count: a program that leaves them out, or rounds other values in their place, can miss the bound.
Values may be sent and summed in bfloat16 or wider, within the bound.
A program may use at most 256 MiB of HBM per device.

```python
import jax
import jax.numpy as jnp
from jax import lax

D = 1536
INNER = 3072
HEADDIM = 64
STATE = 128
CONV = 4
SPAN = 256
H = 48
DOC_LEAST = 200
DOC_MOST = 2000
LEN = 2048
SEQS = 8


def draw_doc_start(key, part):
    count = LEN // DOC_LEAST + 2
    first_key, second_key = jax.random.split(key)
    lengths = jax.random.randint(first_key, (SEQS, count), DOC_LEAST, DOC_MOST + 1)
    chosen = jax.random.randint(second_key, (SEQS, 1), 0, 2)
    column = jnp.arange(count, dtype=jnp.int32)[None, :]
    lengths = jnp.where(column == chosen, DOC_MOST, lengths)
    begins = jnp.cumsum(lengths, axis=1) - lengths
    places = jnp.arange(LEN, dtype=jnp.int32)
    started = begins[:, None, :] <= places[None, :, None]
    starts = jnp.max(jnp.where(started, begins[:, None, :], 0), axis=2).astype(jnp.int32)
    rows = jnp.arange(SEQS, dtype=jnp.int32)[:, None]
    final = (rows == SEQS - 1) & (places[None, :] == LEN - 1)
    return jnp.where(final, LEN - 1, starts).astype(jnp.int32)


def block_scale(rng, dims, cuts, least, largest):
    def one(position, blocks):
        draws = jax.random.uniform(jax.random.fold_in(jax.random.fold_in(rng, 6), position), (blocks,), jnp.float32, least / len(cuts), largest / len(cuts))
        return jnp.repeat(jnp.exp(draws), dims[position] // blocks).reshape((-1,) + (1,) * (len(dims) - position - 1))

    level = one(*cuts[0])
    for cut in cuts[1:]:
        level = level * one(*cut)
    return level


def scatter_about(own_key, dims, deviation, reach, cuts=(), kind=jnp.bfloat16):
    entries = deviation * jax.random.normal(own_key, dims, jnp.float32)
    if cuts:
        entries = entries * block_scale(own_key, dims, cuts, -0.22, 0.18)
    return jnp.clip(entries, -reach, reach).astype(kind)


def setup_inputs(seed: int = 0) -> dict:
    seeds = jax.random.split(jax.random.key(seed), 18)
    tokens = scatter_about(seeds[0], (SEQS, LEN, D), 1.0, 6.0, ((0, 4), (1, 4)))
    cotangent = scatter_about(seeds[1], (SEQS, LEN, D), 1.0, 6.0, ((0, 4), (1, 4)))
    doc_start = draw_doc_start(jax.random.fold_in(seeds[17], 71), 0)
    norm_gain = jnp.clip(jax.random.uniform(seeds[3], (D,), jnp.float32, 0.5, 1.5), 0.5, 1.5)
    gate_proj = scatter_about(seeds[4], (D, INNER), D ** -0.5, 0.15625, ((0, 4), (1, 2)))
    input_proj = scatter_about(seeds[5], (D, INNER), D ** -0.5, 0.15625, ((0, 4), (1, 2)))
    state_proj = scatter_about(seeds[6], (D, 2 * STATE), D ** -0.5, 0.15625, ((0, 4),))
    step_proj = scatter_about(seeds[7], (D, H), D ** -0.5, 0.15625, ((0, 4), (1, 2)))
    inner_kernel = scatter_about(seeds[8], (CONV, INNER), CONV ** -0.5, 3.0, ((1, 2),), jnp.float32)
    inner_shift = scatter_about(seeds[9], (INNER,), 0.5, 3.0, ((0, 2),), jnp.float32)
    state_kernel = scatter_about(seeds[10], (CONV, 2 * STATE), CONV ** -0.5, 3.0, (), jnp.float32)
    state_shift = scatter_about(seeds[11], (2 * STATE,), 0.5, 3.0, (), jnp.float32)
    step_bias = jnp.clip(-4.0 + 3.0 * jax.random.uniform(seeds[12], (H,), jnp.float32) ** block_scale(seeds[12], (H,), ((0, 2),), -0.2, 0.2), -4.0, -1.0)
    decay_log = jnp.clip(-9.0 + 9.5 * jax.random.uniform(seeds[13], (H,), jnp.float32) ** block_scale(seeds[13], (H,), ((0, 2),), -0.2, 0.2), -9.0, 0.5)
    skip_gain = jnp.clip(0.5 + 1.5 * jax.random.uniform(seeds[14], (H,), jnp.float32) ** block_scale(seeds[14], (H,), ((0, 2),), -0.2, 0.2), 0.5, 2.0)
    inner_gain = jnp.clip(0.5 + 1.0 * jax.random.uniform(seeds[15], (INNER,), jnp.float32) ** block_scale(seeds[15], (INNER,), ((0, 2),), -0.2, 0.2), 0.5, 1.5)
    out_proj = scatter_about(seeds[16], (INNER, D), INNER ** -0.5, 0.109375, ((0, 2), (1, 4)))
    return {"tokens": tokens, "cotangent": cotangent, "doc_start": doc_start, "norm_gain": norm_gain, "gate_proj": gate_proj, "input_proj": input_proj, "state_proj": state_proj, "step_proj": step_proj, "inner_kernel": inner_kernel, "inner_shift": inner_shift, "state_kernel": state_kernel, "state_shift": state_shift, "step_bias": step_bias, "decay_log": decay_log, "skip_gain": skip_gain, "inner_gain": inner_gain, "out_proj": out_proj}


@jax.custom_vjp
def low(v):
    return lax.optimization_barrier(v.astype(jnp.bfloat16)).astype(jnp.float32)

@jax.custom_vjp
def low_back(v):
    return v

def low_keep(v):
    return (low(v), None)

def low_pass(kept, grad):
    return (grad,)

def back_keep(v):
    return (v, None)

def back_low(kept, grad):
    return (low(grad),)
low.defvjp(low_keep, low_pass)
low_back.defvjp(back_keep, back_low)
exact = lax.Precision.HIGHEST

def block_step(state, pieces):
    feed, write, read, rate, stride, starts, places = pieces
    total = jnp.cumsum(rate, axis=0)
    first = places[0]
    visible = (starts[:, None] <= places[None, :]) & (places[None, :] <= places[:, None])
    spread = total.T[:, :, None] - total.T[:, None, :]
    fading = jnp.where(visible[None], jnp.exp(jnp.where(visible[None], spread, 0.0)), 0.0)
    intersection = jnp.dot(read, write.T, precision=exact, preferred_element_type=jnp.float32)
    mixing = intersection[None] * fading * stride.T[:, None, :]
    result = jnp.einsum('hts,shp->thp', mixing, feed, precision=exact)
    carried = (starts < first).astype(jnp.float32)
    result = result + jnp.einsum('tn,hpn->thp', read, state, precision=exact) * (jnp.exp(total) * carried[:, None])[:, :, None]
    ending = total[-1]
    tail = (places >= starts[-1]).astype(jnp.float32)
    weights = jnp.exp(ending[None, :] - total) * tail[:, None] * stride
    state = state * (jnp.exp(ending) * carried[-1])[:, None, None] + jnp.einsum('sh,shp,sn->hpn', weights, feed, write, precision=exact)
    return (state, result)

def sequence_scan(feed, write, read, rate, stride, starts):
    blocks = LEN // SPAN
    places = jnp.arange(LEN, dtype=jnp.int32)

    def cutter(value):
        return value.reshape((blocks, SPAN) + value.shape[1:])
    initial = jnp.zeros((H, HEADDIM, STATE), jnp.float32)
    final, result = lax.scan(jax.checkpoint(block_step), initial, (cutter(feed), cutter(write), cutter(read), cutter(rate), cutter(stride), cutter(starts), cutter(places)))
    return result.reshape(LEN, H, HEADDIM)

def layer_sequence(plain, starts, weights):
    norm_gain, gate_proj, input_proj, state_proj, step_proj, inner_kernel, inner_shift, state_kernel, state_shift, step_bias, decay_log, skip_gain, inner_gain, out_proj = weights
    places = jnp.arange(LEN, dtype=jnp.int32)
    factor = lax.rsqrt(lax.optimization_barrier(jnp.mean(plain * plain, axis=1, keepdims=True)) + 1e-05)
    normed = low(plain * factor * norm_gain)
    gate_in = low_back(jnp.dot(normed, gate_proj, precision=exact, preferred_element_type=jnp.float32))
    feed_in = low(low_back(jnp.dot(normed, input_proj, precision=exact, preferred_element_type=jnp.float32)))
    state_in = low(jnp.dot(normed, state_proj, precision=exact, preferred_element_type=jnp.float32))
    step_in = low_back(jnp.dot(normed, step_proj, precision=exact, preferred_element_type=jnp.float32))
    conv_in = jnp.concatenate([feed_in, state_in], axis=1)
    kernel = jnp.concatenate([inner_kernel, state_kernel], axis=1)
    shift = jnp.concatenate([inner_shift, state_shift], axis=0)
    summed = jnp.zeros_like(conv_in) + shift[None, :]
    for index in range(CONV):
        delay = CONV - 1 - index
        moved = jnp.pad(conv_in, ((delay, 0), (0, 0)))[:LEN]
        allowed = (starts <= places - delay).astype(jnp.float32)
        summed = summed + kernel[index][None, :] * moved * allowed[:, None]
    mixed = jax.nn.silu(summed)
    feed = mixed[:, :INNER].reshape(LEN, H, HEADDIM)
    write = mixed[:, INNER:INNER + STATE]
    read = mixed[:, INNER + STATE:]
    stride = jax.nn.softplus(step_in + step_bias)
    rate = -stride * jnp.exp(decay_log)
    mixer_out = sequence_scan(feed, write, read, rate, stride, starts) + skip_gain[None, :, None] * feed
    mixer_out = mixer_out.reshape(LEN, INNER)
    gated = mixer_out * jax.nn.silu(gate_in)
    scale = lax.rsqrt(lax.optimization_barrier(jnp.mean(gated * gated, axis=1, keepdims=True)) + 1e-05)
    inner_out = low(gated * scale * inner_gain)
    return plain + jnp.dot(inner_out, out_proj, precision=exact, preferred_element_type=jnp.float32)

def reference(tokens, cotangent, doc_start, norm_gain, gate_proj, input_proj, state_proj, step_proj, inner_kernel, inner_shift, state_kernel, state_shift, step_bias, decay_log, skip_gain, inner_gain, out_proj):
    weights = tuple((item.astype(jnp.float32) for item in (norm_gain, gate_proj, input_proj, state_proj, step_proj, inner_kernel, inner_shift, state_kernel, state_shift, step_bias, decay_log, skip_gain, inner_gain, out_proj)))

    def forward(plain_all, weights):

        def one(carry, item):
            return (carry, layer_sequence(item[0], item[1], weights))
        unused, outputs = lax.scan(jax.checkpoint(one), jnp.zeros((), jnp.float32), (plain_all, doc_start))
        return outputs
    block_out, pull = jax.vjp(forward, tokens.astype(jnp.float32), weights)
    grad_tokens, grads = pull(cotangent.astype(jnp.float32))
    grad_norm_gain, grad_gate_proj, grad_input_proj, grad_state_proj, grad_step_proj, grad_inner_kernel, grad_inner_shift, grad_state_kernel, grad_state_shift, grad_step_bias, grad_decay_log, grad_skip_gain, grad_inner_gain, grad_out_proj = grads
    return (block_out.astype(jnp.bfloat16), grad_tokens.astype(jnp.bfloat16), grad_norm_gain, grad_gate_proj, grad_input_proj, grad_state_proj, grad_step_proj, grad_inner_kernel, grad_inner_shift, grad_state_kernel, grad_state_shift, grad_step_bias, grad_decay_log, grad_skip_gain, grad_inner_gain, grad_out_proj)
```

```python
import functools

import jax
import jax.numpy as jnp
from jax import lax
from jax.experimental import pallas as pl
from jax.experimental.pallas import tpu as pltpu
from jax.sharding import PartitionSpec as P


BLOCK = 128
GROUP = 8
LANES = 128
MESH = pl.DeviceIdType.MESH
FAR = -1e30
exact = lax.Precision.HIGHEST
f32 = jnp.float32
bf16 = jnp.bfloat16


def cost(us):
    return pl.CostEstimate(flops=int(us * 1.1e9), bytes_accessed=int(us * 3.0e6), transcendentals=0)


def inverse_root(v):
    r = lax.rsqrt(v)
    return r * (1.5 - 0.5 * v * r * r)


def split(x):
    high = x.astype(bf16)
    return high, (x - high.astype(f32)).astype(bf16)


def dots(a, b, ca, cb):
    return dot(a[0], b[0], ca, cb) + (dot(a[1], b[0], ca, cb) + dot(a[0], b[1], ca, cb))


def pair(ref):
    return ref[0], ref[1]


def maps(bc, lanes):
    n = bc.shape[0] // 4
    return (
        (bc[0:n, lanes], bc[2 * n : 3 * n, lanes]),
        (bc[n : 2 * n, lanes], bc[3 * n : 4 * n, lanes]),
    )


def dot(a, b, ca, cb):
    return lax.dot_general(a, b, (((ca,), (cb,)), ((), ())), preferred_element_type=f32)


def shifted(a, axis, distance):
    n = lax.axis_size(axis)
    return lax.ppermute(a, axis, [(i, (i + distance) % n) for i in range(n)])


def from_behind(a, axis, distance):
    devices = range(lax.axis_size(axis))
    return lax.ppermute(a, axis, [(i, i + distance) for i in devices if i + distance in devices])


def core_swap(a):
    return lax.ppermute(a, "dp", [(i, i ^ 1) for i in range(lax.axis_size("dp"))])


def y_shift(a, distance):
    n = lax.axis_size("dp")
    m = n // 2
    return lax.ppermute(
        a, "dp", [(i, ((i // 2 + distance) % m) * 2 + i % 2) for i in range(n)]
    )


def pick(a, index, axis=0):
    return lax.dynamic_index_in_dim(a, index, axis, False)


def assemble(sources, pieces, shape):
    lead = len(shape) - 2

    def body(*refs):
        where, ins, out = refs[0], refs[1:-1], refs[-1]
        for i in range(len(pieces)):
            at = tuple(where[i * lead + k] for k in range(lead))
            column = sources[i][1]
            out[at + (slice(None), slice(column, column + ins[i].shape[1]))] = ins[i][...]

    table = [jnp.asarray(v, jnp.int32) for source in sources for v in source[0]]
    return pl.pallas_call(
        body,
        out_shape=jax.ShapeDtypeStruct(shape, pieces[0].dtype),
        in_specs=[pl.BlockSpec(memory_space=pltpu.SMEM)]
        + [pl.BlockSpec(memory_space=pltpu.VMEM)] * len(pieces),
        out_specs=pl.BlockSpec(memory_space=pltpu.VMEM),
        compiler_params=pltpu.CompilerParams(vmem_limit_bytes=40 << 20),
        cost_estimate=cost(3.0),
        name="assemble",
    )(jnp.stack(table), *pieces)


def gather_kernel(nz, ny, many, *refs):
    shards, (tokens, tail, cotangent, gain) = refs[:many], refs[many : many + 4]
    fulls = refs[many + 4 : 2 * many + 4]
    ext, up, normed_half, up_half, own, z_send, z_recv, y_send, y_recv, c_send, c_recv = refs[2 * many + 4 :]
    z, d = lax.axis_index("seq"), lax.axis_index("dp")
    y, core = d // 2, lax.rem(d, 2)

    def along_z(hop):
        return {"seq": lax.rem(z + hop, nz)}

    def along_y(step):
        return {"dp": lax.rem(y + step, ny) * 2 + core}

    other = {"dp": y * 2 + 1 - core}
    peers = [along_z(h) for h in range(1, nz)] + [along_y(s) for s in range(1, ny)] + [other]
    barrier = pltpu.get_barrier_semaphore()
    for peer in peers:
        pl.semaphore_signal(barrier, inc=1, device_id=peer, device_id_type=MESH)
    pl.semaphore_wait(barrier, len(peers))

    def copy(src, dst, send, recv, peer):
        return pltpu.make_async_remote_copy(
            src_ref=src, dst_ref=dst, send_sem=send, recv_sem=recv, device_id=peer, device_id_type=MESH
        )

    def z_copy(p, hop):
        return copy(
            shards[p].at[core, y], fulls[p].at[z, core, y], z_send.at[p, hop], z_recv.at[p, hop], along_z(hop)
        )

    def place(p, hop, row):
        return fulls[p].at[lax.rem(z + nz - hop, nz), core, row]

    def y_copy(p, hop, step):
        at = place(p, hop, y)
        return copy(at, at, y_send.at[p, hop, step], y_recv.at[p, hop, step], along_y(step))

    def c_copy(p, hop, step):
        at = place(p, hop, lax.rem(y + ny - step, ny))
        return copy(at, at, c_send.at[p, hop, step], c_recv.at[p, hop, step], other)

    hops = range(1, nz)
    for p in range(many):
        for hop in hops:
            z_copy(p, hop).start()
    for p in range(many):
        pltpu.make_async_copy(shards[p], fulls[p].at[z], own.at[p]).start()

    width = tokens.shape[1]
    blocks = tokens.shape[0] // LANES
    part = width // (2 * nz)

    def norm(rows):
        plain = rows.astype(f32)
        factor = inverse_root(jnp.mean(plain * plain, axis=1, keepdims=True) + 1e-05)
        return (plain * factor * gain[...]).astype(bf16)

    def prepare(i, _):
        at = pl.ds(pl.multiple_of(i * LANES, LANES), LANES)
        for value, whole, half in ((norm(tokens[at, :]), ext, normed_half), (cotangent[at, :], up, up_half)):
            turned = jnp.transpose(value)
            whole[:, at] = turned
            for block in range(2 * nz):
                side = lax.rem(core + block, 2)
                half[side, block // 2 * part : (block // 2 + 1) * part, at] = turned[
                    block * part : (block + 1) * part, :
                ]
        return 0

    lax.fori_loop(0, blocks, prepare, 0)

    def prepare_tail(i, _):
        at = pl.ds(pl.multiple_of(i * LANES, LANES), LANES)
        to = pl.ds(pl.multiple_of((blocks + i) * LANES, LANES), LANES)
        ext[:, to] = jnp.transpose(norm(tail[at, :]))
        return 0

    lax.fori_loop(0, tail.shape[0] // LANES, prepare_tail, 0)
    for p in range(many):
        for hop in hops:
            z_copy(p, hop).wait_recv()
            for step in range(1, ny):
                y_copy(p, hop, step).start()
            c_copy(p, hop, 0).start()
        for hop in hops:
            for step in range(1, ny):
                y_copy(p, hop, step).wait_recv()
                c_copy(p, hop, step).start()
    for p in range(many):
        pltpu.make_async_copy(shards[p], fulls[p].at[z], own.at[p]).wait()
        for hop in hops:
            z_copy(p, hop).wait_send()
            for step in range(1, ny):
                y_copy(p, hop, step).wait_send()
            for step in range(ny):
                c_copy(p, hop, step).wait()


def begin(shards, tokens, tail, cotangent, gain):
    nz, nd = lax.axis_size("seq"), lax.axis_size("dp")
    ny = nd // 2
    many = len(shards)
    split = [a.reshape(2, ny, a.shape[0] // nd, a.shape[1]) for a in shards]
    sems = [(many,), (many, nz), (many, nz), (many, nz, ny), (many, nz, ny), (many, nz, ny), (many, nz, ny)]
    count, width = tokens.shape
    vmem = pl.BlockSpec(memory_space=pltpu.VMEM)
    outs = pl.pallas_call(
        functools.partial(gather_kernel, nz, ny, many),
        out_shape=[jax.ShapeDtypeStruct((nz,) + a.shape, a.dtype) for a in split]
        + [
            jax.ShapeDtypeStruct((width, count + tail.shape[0]), bf16),
            jax.ShapeDtypeStruct((width, count), bf16),
            jax.ShapeDtypeStruct((2, width // 2, count), bf16),
            jax.ShapeDtypeStruct((2, width // 2, count), bf16),
        ],
        in_specs=[vmem] * (many + 4),
        out_specs=[pl.BlockSpec(memory_space=pl.ANY)] * many + [vmem] * 4,
        scratch_shapes=[pltpu.SemaphoreType.DMA(shape) for shape in sems],
        compiler_params=pltpu.CompilerParams(
            collective_id=0, has_side_effects=True, vmem_limit_bytes=56 << 20
        ),
        name="gather",
    )(*split, tokens, tail, cotangent, gain)
    fulls = [full.reshape(nz * a.shape[0], a.shape[1]) for full, a in zip(outs, shards)]
    return fulls, outs[many:]


def all_sum(a, *axes):
    for axis in axes:
        n = lax.axis_size(axis)
        bit = 1
        while bit < n:
            a = a + lax.ppermute(a, axis, [(i, i ^ bit) for i in range(n)])
            bit *= 2
    return a


def reduction(theirs, mine, right, low=None, kind=bf16):
    nz, nd = lax.axis_size("seq"), lax.axis_size("dp")
    ny = nd // 2
    z, d = lax.axis_index("seq"), lax.axis_index("dp")
    y = d // 2

    def product(left):
        full = dot(left, right, 1, 1)
        return full if low is None else full + dot(left, low, 1, 1)

    first = product(theirs)
    yield first
    summed = product(mine) + core_swap(first)
    summed = summed.reshape(nz, ny, -1, summed.shape[1])
    sends = [pick(summed, (y + step) % ny, 1).astype(kind) for step in range(1, ny)]
    own = pick(summed, y, 1)
    yield sends
    for step in range(1, ny):
        own = own + y_shift(sends[step - 1], step).astype(f32)
    sends = [pick(own, (z + step) % nz).astype(kind) for step in range(1, nz)]
    total = pick(own, z)
    yield sends
    for step in range(1, nz):
        total = total + shifted(sends[step - 1], "seq", step).astype(f32)
    yield total


def fence(value, *others):
    return lax.optimization_barrier((value, others))[0]


def spread_rows(totals):
    nd = lax.axis_size("dp")
    ny = nd // 2
    d = lax.axis_index("dp")
    y, core = d // 2, d % 2
    pieces, sources, column = [], [], 0
    for total in totals:
        held = [(y, total)]
        for step in range(1, ny):
            held.append(((y - step) % ny, y_shift(total, step)))
        for row, piece in held:
            pieces.append(piece)
            sources.append(((core, row), column))
            pieces.append(core_swap(piece))
            sources.append(((1 - core, row), column))
        column += total.shape[1]
    r = totals[0].shape[0]
    return assemble(sources, pieces, (2, ny, r, column)).reshape(nd * r, column)


def chain_states(value, fading, reverse):
    n = lax.axis_size("seq")
    came = jnp.zeros(value.shape, f32)
    for hop in range(1, n):
        send = (value.astype(f32) + fading * came.astype(f32)).astype(f32) if hop > 1 else value
        came = from_behind(send, "seq", -1 if reverse else 1)
    return came


def row_iota(n):
    return lax.broadcasted_iota(jnp.int32, (1, n), 1)


def allowed_rows(starts, length):
    places = row_iota(length)
    return [None] + [(starts <= places - delay).astype(f32) for delay in (1, 2, 3)]


def conv_rows(x, halo, taps, allowed):
    x = x.astype(f32)
    joined = jnp.concatenate([halo.astype(f32), x], axis=1)
    pre = taps[:, 4:5] + taps[:, 3:4] * x
    moved = [x]
    for delay in (1, 2, 3):
        m = pltpu.roll(joined, delay, 1)[:, LANES:] * allowed[delay]
        moved.append(m)
        pre = pre + taps[:, 3 - delay : 4 - delay] * m
    return pre, moved


def conv_back(grad, moved, taps, allowed):
    rows, length = grad.shape
    lane = lax.broadcasted_iota(jnp.int32, (rows, LANES), 1)
    joined = jnp.zeros((rows, LANES + length), f32)
    sums = jnp.where(lane == 4, jnp.sum(grad, axis=1, keepdims=True), 0.0)
    blank = jnp.zeros((rows, LANES), f32)
    for delay in range(4):
        part = jnp.sum(grad * moved[delay], axis=1, keepdims=True)
        sums = jnp.where(lane == 3 - delay, part, sums)
        v = taps[:, 3 - delay : 4 - delay] * grad
        if delay:
            v = v * allowed[delay]
        v = jnp.concatenate([blank, v], axis=1)
        if delay:
            v = pltpu.roll(v, LANES + length - delay, 1)
        joined = joined + v
    return joined, sums


def block_masks(starts, c):
    s = lax.broadcasted_iota(jnp.int32, (BLOCK, BLOCK), 0) + c * BLOCK
    t = lax.broadcasted_iota(jnp.int32, (BLOCK, BLOCK), 1) + c * BLOCK
    row = row_iota(BLOCK) + c * BLOCK
    last = starts[:, BLOCK - 1 : BLOCK]
    visible = jnp.where((starts <= s) & (s <= t), 0.0, FAR)
    carried = jnp.where(starts < c * BLOCK, 0.0, FAR)
    tail = jnp.where(row >= last, 0.0, FAR)
    carried_last = jnp.where(last < c * BLOCK, 0.0, FAR)
    return visible, carried, tail, carried_last


def column(row):
    return jnp.transpose(jnp.broadcast_to(row, (BLOCK, BLOCK)))


def local_kernel(x, hx, st, hst, taps, taps_st, starts, tot, stride, skip, y, end, bc, xs, state, inter, weighted):
    length = x.shape[1]
    rows = x.shape[0] // GROUP
    allowed = allowed_rows(starts[...], length)

    @pl.when(pl.program_id(0) == 0)
    def _():
        def one(i, _):
            at = pl.ds(pl.multiple_of(i * 64, 64), 64)
            pre, _m = conv_rows(st[at, :], hst[at, :], taps_st[at, :], allowed)
            high, low = split(pre * jax.nn.sigmoid(pre))
            bc[at, :] = high
            bc[pl.ds(pl.multiple_of(st.shape[0] + i * 64, 64), 64), :] = low
            return 0

        lax.fori_loop(0, st.shape[0] // 64, one, 0)

    def conv(i, _):
        at = pl.ds(pl.multiple_of(i * rows, rows), rows)
        pre, _m = conv_rows(x[at, :], hx[at, :], taps[at, :], allowed)
        xs[at, :] = pre * jax.nn.sigmoid(pre)
        return 0

    lax.fori_loop(0, GROUP, conv, 0)
    state[...] = jnp.zeros_like(state)

    def block(c, _):
        lanes = pl.ds(pl.multiple_of(c * BLOCK, BLOCK), BLOCK)
        write, read = maps(bc, lanes)
        cross = dots(write, read, 0, 0)
        visible, carried, tail, carried_last = block_masks(starts[:, lanes], c)
        inter[...] = dots(split(state[...]), read, 1, 0)
        for h in range(GROUP):
            at = slice(h * rows, (h + 1) * rows)
            total = tot[h : h + 1, lanes]
            ending = total[:, BLOCK - 1 : BLOCK]
            fade = jnp.exp(total - column(total) + visible)
            mixing = (cross * fade).astype(bf16)
            feed = xs[at, lanes]
            scaled = feed * stride[h : h + 1, lanes]
            y[at, lanes] = (
                dot(scaled.astype(bf16), mixing, 1, 0)
                + inter[at, :] * jnp.exp(total + carried)
                + skip[h : h + 1, :] * feed
            )
            for k, term in enumerate(split(scaled * jnp.exp(ending - total + tail))):
                weighted[k, at, :] = term
            state[at, :] = state[at, :] * jnp.exp(ending + carried_last)
        state[...] += dots(pair(weighted), write, 1, 1)
        return 0

    lax.fori_loop(0, length // BLOCK, block, 0)
    end[...] = state[...]


def join_kernel(y, entering, read, read_low, edev, gate, grad_inner, taps, mixer, sums, inter):
    rows = y.shape[0] // GROUP

    @pl.when(pl.program_id(0) == 0)
    def _():
        sums[...] = jnp.zeros_like(sums)

    inter[...] = dots(split(entering[...]), (read[...], read_low[...]), 1, 0)

    def one(h, total):
        at = pl.ds(pl.multiple_of(h * rows, rows), rows)
        m = y[at, :] + inter[at, :] * edev[pl.ds(h, 1), :]
        mixer[at, :] = m
        g = gate[at, :]
        gated = m * (g * jax.nn.sigmoid(g))
        square = jnp.sum(gated * gated, axis=0, keepdims=True)
        product = jnp.sum(grad_inner[at, :] * taps[at, 5:6] * gated, axis=0, keepdims=True)
        return total[0] + square, total[1] + product

    zero = jnp.zeros((1, y.shape[1]), f32)
    square, product = lax.fori_loop(0, GROUP, one, (zero, zero))
    sums[0:1, :] += square
    sums[1:2, :] += product


def gate_kernel(inner_total, aliased, *refs):
    mixer, gate, grad_inner, own, came, edev, read, read_low, taps = refs[:9]
    inner_out, grad_mixer, grad_gate, grad_entering, grad_gain, faded = refs[9 + 2 * aliased :]
    rows = mixer.shape[0] // GROUP
    summed = own[0:2, :] + came[0:2, :]
    scale = inverse_root(summed[0:1, :] / inner_total + 1e-05)
    back = scale * scale * scale * (summed[1:2, :] / inner_total)

    def one(h, _):
        at = pl.ds(pl.multiple_of(h * rows, rows), rows)
        m, g, gi = mixer[at, :], gate[at, :], grad_inner[at, :]
        sigma = jax.nn.sigmoid(g)
        opened = g * sigma
        gated = m * opened
        gain = taps[at, 5:6]
        normal = gated * scale
        inner_out[at, :] = (normal * gain).astype(bf16)
        grad_gain[at, :] = jnp.broadcast_to(jnp.sum(gi * normal, axis=1, keepdims=True), (rows, LANES))
        grad_gated = scale * (gi * gain) - gated * back
        gm = grad_gated * opened
        grad_mixer[at, :] = gm
        grad_gate[at, :] = (grad_gated * m * sigma * (1.0 + g * (1.0 - sigma))).astype(bf16)
        for k, term in enumerate(split(gm * edev[pl.ds(h, 1), :])):
            faded[k, at, :] = term
        return 0

    lax.fori_loop(0, GROUP, one, 0)
    grad_entering[...] = dots(pair(faded), (read[...], read_low[...]), 1, 1)


def back_kernel(first, last, *refs):
    (x, hx, taps, starts, tot, stride, skip, grad_mixer, entering, later, bc) = refs[:11]
    if not first:
        gbc_before, gcross_before = refs[11:13]
    at_out = 11 if first else 13
    (gx, ghalo, gtaps, gstride, gtot, gskip, gbc, gcross) = refs[at_out : at_out + 8]
    xs, slope, gfeed, states, state, gstate, cross_from, cross_to, weighted, faded = refs[at_out + 8 :]
    length = x.shape[1]
    rows = x.shape[0] // GROUP
    n = bc.shape[0] // 4
    blocks = length // BLOCK
    allowed = allowed_rows(starts[...], length)
    if first:
        gbc[...] = jnp.zeros_like(gbc)
        gcross[...] = jnp.zeros_like(gcross)
    else:
        gbc[...] = gbc_before[...]
        gcross[...] = gcross_before[...]

    def conv(i, _):
        at = pl.ds(pl.multiple_of(i * rows, rows), rows)
        pre, _m = conv_rows(x[at, :], hx[at, :], taps[at, :], allowed)
        s = jax.nn.sigmoid(pre)
        xs[at, :] = pre * s
        slope[at, :] = s * (1.0 + pre * (1.0 - s))
        return 0

    lax.fori_loop(0, GROUP, conv, 0)
    state[...] = entering[...].astype(f32)

    def ahead(c, _):
        lanes = pl.ds(pl.multiple_of(c * BLOCK, BLOCK), BLOCK)
        for k, term in enumerate(split(state[...])):
            states[k, c] = term
        _v, _c, tail, carried_last = block_masks(starts[:, lanes], c)
        for h in range(GROUP):
            at = slice(h * rows, (h + 1) * rows)
            total = tot[h : h + 1, lanes]
            ending = total[:, BLOCK - 1 : BLOCK]
            scaled = xs[at, lanes] * stride[h : h + 1, lanes]
            for k, term in enumerate(split(scaled * jnp.exp(ending - total + tail))):
                weighted[k, at, :] = term
            state[at, :] = state[at, :] * jnp.exp(ending + carried_last)
        state[...] += dots(pair(weighted), maps(bc, lanes)[0], 1, 1)
        return 0

    lax.fori_loop(0, blocks - 1, ahead, 0)
    for k, term in enumerate(split(state[...])):
        states[k, blocks - 1] = term
    gstate[...] = later[...].astype(f32)
    ones = jnp.ones((8, BLOCK), bf16)
    lastlane = row_iota(BLOCK) == BLOCK - 1

    def block(i, _):
        c = blocks - 1 - i
        lanes = pl.ds(pl.multiple_of(c * BLOCK, BLOCK), BLOCK)
        write, read = maps(bc, lanes)
        cross = dots(write, read, 0, 0)
        visible, carried, tail, carried_last = block_masks(starts[:, lanes], c)
        before = (states[0, c], states[1, c])
        after = split(gstate[...])
        cross_from[...] = dot(before[0], read[0], 1, 0)
        cross_to[...] = dot(after[0], write[0], 1, 0)
        mixed = jnp.zeros((BLOCK, BLOCK), f32)
        for h in range(GROUP):
            at = slice(h * rows, (h + 1) * rows)
            total = tot[h : h + 1, lanes]
            ending = total[:, BLOCK - 1 : BLOCK]
            fade = jnp.exp(total - column(total) + visible)
            enter = jnp.exp(total + carried)
            weight = jnp.exp(ending - total + tail)
            decay = jnp.exp(ending + carried_last)
            feed = xs[at, lanes]
            pace = stride[h : h + 1, lanes]
            scaled = feed * pace
            gm = grad_mixer[at, lanes]
            gms = split(gm)
            outer = dots(split(scaled), gms, 0, 0) * fade
            mixed = mixed + outer
            pairs = (outer * cross).astype(bf16)
            mixing = (cross * fade).astype(bf16)
            leaving = cross_to[at, :] * weight
            reach = dot(gms[0], mixing, 1, 1) + leaving
            gfeed[at, lanes] = pace * reach + skip[h : h + 1, :] * gm
            gstride[h : h + 1, lanes] = jnp.sum(feed * reach, axis=0, keepdims=True)
            left = jnp.sum(scaled * leaving, axis=0, keepdims=True)
            came = jnp.sum(gm * cross_from[at, :], axis=0, keepdims=True) * enter
            into = jnp.sum(pairs.astype(f32), axis=0, keepdims=True)
            out = dot(ones, pairs, 1, 1)[0:1, :]
            held = gstate[at, :]
            flux = jnp.sum(
                jnp.sum(before[0][at, :].astype(f32) * held, axis=0, keepdims=True), axis=1, keepdims=True
            )
            final = jnp.sum(left, axis=1, keepdims=True) + flux * decay
            gtot[h : h + 1, lanes] = into - out + came - left + jnp.where(lastlane, final, 0.0)
            dskip = jnp.sum(gm * feed, axis=0, keepdims=True)
            gskip[h : h + 1, :] = jnp.where(i == 0, dskip, gskip[h : h + 1, :] + dskip)
            for k, term in enumerate(split(gm * enter)):
                faded[k, at, :] = term
            for k, term in enumerate(split(scaled * weight)):
                weighted[k, at, :] = term
            gstate[at, :] = held * decay
        gcross[c] += mixed
        gbc[n : 2 * n, lanes] += dots(before, pair(faded), 0, 0)
        gbc[0:n, lanes] += dots(after, pair(weighted), 0, 0)
        gstate[...] += dots(pair(faded), read, 1, 1)
        return 0

    lax.fori_loop(0, blocks, block, 0)

    def conv_grad(i, _):
        at = pl.ds(pl.multiple_of(i * rows, rows), rows)
        _p, moved = conv_rows(x[at, :], hx[at, :], taps[at, :], allowed)
        joined, sums = conv_back(gfeed[at, :] * slope[at, :], moved, taps[at, :], allowed)
        gx[at, :] = joined[:, LANES:].astype(bf16)
        ghalo[at, :] = joined[:, :LANES].astype(bf16)
        gtaps[at, :] = sums
        return 0

    lax.fori_loop(0, GROUP, conv_grad, 0)

    if last:

        def one(c, _):
            lanes = pl.ds(pl.multiple_of(c * BLOCK, BLOCK), BLOCK)
            write, read = maps(bc, lanes)
            terms = split(gcross[c])
            gbc[n : 2 * n, lanes] += dots(write, terms, 1, 0)
            gbc[0:n, lanes] += dots(read, terms, 1, 1)
            return 0

        lax.fori_loop(0, blocks, one, 0)


def state_back_kernel(st, hst, taps, starts, gbc, gst, ghalo, gtaps):
    length = st.shape[1]
    allowed = allowed_rows(starts[...], length)

    def one(i, _):
        at = pl.ds(pl.multiple_of(i * 64, 64), 64)
        pre, moved = conv_rows(st[at, :], hst[at, :], taps[at, :], allowed)
        s = jax.nn.sigmoid(pre)
        grad = gbc[at, :] * (s * (1.0 + pre * (1.0 - s)))
        joined, sums = conv_back(grad, moved, taps[at, :], allowed)
        gst[at, :] = joined[:, LANES:]
        ghalo[at, :] = joined[:, :LANES]
        gtaps[at, :] = sums
        return 0

    lax.fori_loop(0, st.shape[0] // 64, one, 0)


def params():
    return pltpu.CompilerParams(vmem_limit_bytes=48 << 20)


def per_device(
    tokens,
    cotangent,
    doc_start,
    norm_gain,
    gate_proj,
    input_proj,
    state_proj,
    step_proj,
    inner_kernel,
    inner_shift,
    state_kernel,
    state_shift,
    step_bias,
    decay_log,
    skip_gain,
    inner_gain,
    out_proj,
):
    groups, length, width = tokens.shape
    count = groups * length
    heads = step_bias.shape[0]
    inner = inner_gain.shape[0]
    headsize = inner // heads
    n = state_kernel.shape[1] // 2
    chunk = GROUP * headsize
    steps = heads // GROUP
    blocks = length // BLOCK
    inner_total = inner * lax.axis_size("head")

    small = 2 * n + heads
    pad = -small % LANES
    packed = jnp.concatenate(
        [input_proj, state_proj, step_proj, jnp.zeros((input_proj.shape[0], pad), bf16)], axis=1
    )
    tail = from_behind(tokens[:, length - 3 :, :], "seq", 1)
    tail = jnp.pad(tail, ((0, 0), (LANES - 3, 0), (0, 0))).reshape(groups * LANES, width)
    upstream = cotangent.reshape(count, width)
    (full, gate_full, out_full), (ext, up_t, normed_half, up_half) = begin(
        [packed, gate_proj, out_proj.T], tokens.reshape(count, width), tail, upstream, norm_gain[None]
    )
    normed_mine, normed_theirs = normed_half[0], normed_half[1]
    up_mine, up_theirs = up_half[0], up_half[1]
    plain = tokens.reshape(count, width).astype(f32)

    starts = doc_start - lax.axis_index("seq") * length
    starts_row = starts.reshape(1, count)
    taps = jnp.concatenate(
        [
            jnp.concatenate([inner_kernel, state_kernel], axis=1),
            jnp.concatenate([inner_shift, state_shift])[None],
            jnp.concatenate([inner_gain, jnp.zeros((2 * n,), f32)])[None],
            jnp.zeros((2, inner + 2 * n), f32),
        ],
        axis=0,
    ).T
    skip_rows = jnp.broadcast_to(skip_gain[:, None], (heads, LANES))

    proj = dot(full[:, : inner + 2 * n], ext, 0, 0).astype(bf16)
    step_in = dot(full[:, inner + 2 * n :], ext[:, :count], 0, 0)[:heads]
    biased = step_in + step_bias[:, None]
    stride = jax.nn.softplus(biased)
    pace = jnp.exp(decay_log)[:, None]
    rate = -stride * pace
    upto = jnp.triu(jnp.ones((BLOCK, BLOCK), f32))
    tot3 = jnp.einsum("hks,st->hkt", rate.reshape(heads, groups * blocks, BLOCK), upto, precision=exact)
    tot = tot3.reshape(heads, count)
    ends = tot3[:, :, BLOCK - 1].reshape(heads, groups, blocks)
    before = jnp.cumsum(ends, axis=2) - ends
    from_start = tot.reshape(heads, groups, blocks, BLOCK) + before[..., None]
    edev = jnp.where((starts < 0)[None], jnp.exp(from_start.reshape(heads, groups, length)), 0.0)
    edev = edev.reshape(heads, count)
    fading = jnp.where(starts[None, :, -1] < 0, jnp.exp(jnp.sum(ends, axis=2)), 0.0)
    fading = jnp.repeat(fading, headsize, axis=0)

    halo_at = count // LANES
    grid = (steps,)

    def spec(shape, where):
        return pl.BlockSpec(shape, where)

    def local(g):
        return pl.pallas_call(
            local_kernel,
            grid=grid,
            in_specs=[
                spec((chunk, length), lambda i: (i, g)),
                spec((chunk, LANES), lambda i: (i, halo_at + g)),
                spec((2 * n, length), lambda i: (inner // (2 * n), g)),
                spec((2 * n, LANES), lambda i: (inner // (2 * n), halo_at + g)),
                spec((chunk, 8), lambda i: (i, 0)),
                spec((2 * n, 8), lambda i: (inner // (2 * n), 0)),
                spec((1, length), lambda i: (0, g)),
                spec((GROUP, length), lambda i: (i, g)),
                spec((GROUP, length), lambda i: (i, g)),
                spec((GROUP, LANES), lambda i: (i, 0)),
            ],
            out_specs=[
                spec((chunk, length), lambda i: (i, 0)),
                spec((chunk, n), lambda i: (i, 0)),
                spec((4 * n, length), lambda i: (0, 0)),
            ],
            out_shape=[
                jax.ShapeDtypeStruct((inner, length), f32),
                jax.ShapeDtypeStruct((inner, n), f32),
                jax.ShapeDtypeStruct((4 * n, length), bf16),
            ],
            scratch_shapes=[
                pltpu.VMEM((chunk, length), f32),
                pltpu.VMEM((chunk, n), f32),
                pltpu.VMEM((chunk, BLOCK), f32),
                pltpu.VMEM((2, chunk, BLOCK), bf16),
            ],
            compiler_params=params(),
            cost_estimate=cost(12.5),
            name="local",
        )(proj, proj, proj, proj, taps, taps, starts_row, tot, stride, skip_rows)

    locals_ = [local(g) for g in range(groups)]
    entering = [chain_states(locals_[g][1], fading[:, g : g + 1], False) for g in range(groups)]
    gate_in = dot(gate_full, ext[:, :count], 0, 0)
    grad_inner = dot(out_full, up_t, 0, 0)

    def join(g):
        return pl.pallas_call(
            join_kernel,
            grid=grid,
            in_specs=[
                spec((chunk, length), lambda i: (i, 0)),
                spec((chunk, n), lambda i: (i, 0)),
                spec((n, length), lambda i: (1, 0)),
                spec((n, length), lambda i: (3, 0)),
                spec((GROUP, length), lambda i: (i, g)),
                spec((chunk, length), lambda i: (i, g)),
                spec((chunk, length), lambda i: (i, g)),
                spec((chunk, 8), lambda i: (i, 0)),
            ],
            out_specs=[
                spec((chunk, length), lambda i: (i, 0)),
                spec((8, length), lambda i: (0, 0)),
            ],
            out_shape=[
                jax.ShapeDtypeStruct((inner, length), f32),
                jax.ShapeDtypeStruct((8, length), f32),
            ],
            scratch_shapes=[pltpu.VMEM((chunk, length), f32)],
            compiler_params=params(),
            cost_estimate=cost(6),
            name="join",
        )(locals_[g][0], entering[g], locals_[g][2], locals_[g][2], edev, gate_in, grad_inner, taps)

    joined = [join(g) for g in range(groups)]
    came = [shifted(joined[g][1], "head", 1) for g in range(groups)]

    def gating(g, carried):
        aliased = len(carried)
        return pl.pallas_call(
            functools.partial(gate_kernel, inner_total, aliased // 2),
            grid=grid,
            in_specs=[
                spec((chunk, length), lambda i: (i, 0)),
                spec((chunk, length), lambda i: (i, g)),
                spec((chunk, length), lambda i: (i, g)),
                spec((8, length), lambda i: (0, 0)),
                spec((8, length), lambda i: (0, 0)),
                spec((GROUP, length), lambda i: (i, g)),
                spec((n, length), lambda i: (1, 0)),
                spec((n, length), lambda i: (3, 0)),
                spec((chunk, 8), lambda i: (i, 0)),
            ]
            + [pl.BlockSpec(memory_space=pl.ANY)] * aliased,
            out_specs=[
                spec((chunk, length), lambda i: (i, g)),
                spec((chunk, length), lambda i: (i, 0)),
                spec((chunk, length), lambda i: (i, g)),
                spec((chunk, n), lambda i: (i, 0)),
                spec((chunk, LANES), lambda i: (i, 0)),
            ],
            out_shape=[
                jax.ShapeDtypeStruct((inner, count), bf16),
                jax.ShapeDtypeStruct((inner, length), f32),
                jax.ShapeDtypeStruct((inner, count), bf16),
                jax.ShapeDtypeStruct((inner, n), f32),
                jax.ShapeDtypeStruct((inner, LANES), f32),
            ],
            scratch_shapes=[pltpu.VMEM((2, chunk, length), bf16)],
            input_output_aliases={9: 0, 10: 2} if aliased else {},
            compiler_params=params(),
            cost_estimate=cost(9),
            name="gating",
        )(joined[g][0], gate_in, grad_inner, joined[g][1], came[g], edev, locals_[g][2], locals_[g][2], taps, *carried)

    gated, carried = [], ()
    for g in range(groups):
        gated.append(gating(g, carried))
        carried = (gated[g][0], gated[g][2])
    inner_out, grad_gate_in = carried
    later = [chain_states(gated[g][3], fading[:, g : g + 1], True) for g in range(groups)]
    grad_inner_gain = sum(gated[g][4][:, 0] for g in range(groups))

    branch = dot(inner_out, out_full, 0, 1).astype(bf16)
    branch_came = shifted(branch, "head", 1)
    block_out = (plain + (branch.astype(f32) + branch_came.astype(f32))).astype(bf16)
    block_out = block_out.reshape(groups, length, width)

    out_sum = reduction(up_theirs, up_mine, inner_out)
    gate_sum = reduction(normed_theirs, normed_mine, grad_gate_in)

    def back(g, i, skip_rows, sums):
        at = lambda *where: (lambda _: where)
        return pl.pallas_call(
            functools.partial(back_kernel, i == 0, i == steps - 1),
            grid=(1,),
            in_specs=[
                spec((chunk, length), at(i, g)),
                spec((chunk, LANES), at(i, halo_at + g)),
                spec((chunk, 8), at(i, 0)),
                spec((1, length), at(0, g)),
                spec((GROUP, length), at(i, g)),
                spec((GROUP, length), at(i, g)),
                spec((GROUP, LANES), at(i, 0)),
                spec((chunk, length), at(i, 0)),
                spec((chunk, n), at(i, 0)),
                spec((chunk, n), at(i, 0)),
                spec((4 * n, length), at(0, 0)),
            ]
            + [spec((2 * n, length), at(0, 0)), spec((blocks, BLOCK, BLOCK), at(0, 0, 0))][: len(sums)],
            out_specs=[
                spec((chunk, length), at(0, 0)),
                spec((chunk, LANES), at(0, 0)),
                spec((chunk, LANES), at(0, 0)),
                spec((GROUP, length), at(0, 0)),
                spec((GROUP, length), at(0, 0)),
                spec((GROUP, LANES), at(0, 0)),
                spec((2 * n, length), at(0, 0)),
                spec((blocks, BLOCK, BLOCK), at(0, 0, 0)),
            ],
            out_shape=[
                jax.ShapeDtypeStruct((chunk, length), bf16),
                jax.ShapeDtypeStruct((chunk, LANES), bf16),
                jax.ShapeDtypeStruct((chunk, LANES), f32),
                jax.ShapeDtypeStruct((GROUP, length), f32),
                jax.ShapeDtypeStruct((GROUP, length), f32),
                jax.ShapeDtypeStruct((GROUP, LANES), f32),
                jax.ShapeDtypeStruct((2 * n, length), f32),
                jax.ShapeDtypeStruct((blocks, BLOCK, BLOCK), f32),
            ],
            scratch_shapes=[
                pltpu.VMEM((chunk, length), f32),
                pltpu.VMEM((chunk, length), f32),
                pltpu.VMEM((chunk, length), f32),
                pltpu.VMEM((2, blocks, chunk, n), bf16),
                pltpu.VMEM((chunk, n), f32),
                pltpu.VMEM((chunk, n), f32),
                pltpu.VMEM((chunk, BLOCK), f32),
                pltpu.VMEM((chunk, BLOCK), f32),
                pltpu.VMEM((2, chunk, BLOCK), bf16),
                pltpu.VMEM((2, chunk, BLOCK), bf16),
            ],
            compiler_params=params(),
            cost_estimate=cost(14),
            name="back",
        )(
            proj, proj, taps, starts_row, tot, stride, skip_rows,
            gated[g][1], entering[g], later[g], locals_[g][2], *sums,
        )

    def state_back(g):
        return pl.pallas_call(
            state_back_kernel,
            grid=(1,),
            in_specs=[
                spec((2 * n, length), lambda i: (inner // (2 * n), g)),
                spec((2 * n, LANES), lambda i: (inner // (2 * n), halo_at + g)),
                spec((2 * n, 8), lambda i: (inner // (2 * n), 0)),
                spec((1, length), lambda i: (0, g)),
                spec((2 * n, length), lambda i: (0, 0)),
            ],
            out_specs=[
                spec((2 * n, length), lambda i: (0, 0)),
                spec((2 * n, LANES), lambda i: (0, 0)),
                spec((2 * n, LANES), lambda i: (0, 0)),
            ],
            out_shape=[
                jax.ShapeDtypeStruct((2 * n, length), f32),
                jax.ShapeDtypeStruct((2 * n, LANES), f32),
                jax.ShapeDtypeStruct((2 * n, LANES), f32),
            ],
            compiler_params=params(),
            cost_estimate=cost(3),
            name="state_back",
        )(proj, proj, taps, starts_row, sums[g][0])

    def returned(halo):
        return from_behind(halo[:, LANES - 3 :], "seq", -1)

    def with_returned(a, came):
        start = length - LANES
        block = lax.slice_in_dim(a, start, start + LANES, axis=1).astype(f32)
        block = block + jnp.pad(came.astype(f32), ((0, 0), (LANES - 3, 0)))
        return lax.dynamic_update_slice_in_dim(a, block.astype(bf16), start, 1)

    def dots_of(g, gx, small):
        def body(wg, wf, gg, x0, x1, x2, sm, out):
            columns = wg.shape[1]
            total = dot(wg[...], gg[...], 1, 0)
            for k, ref in enumerate((x0, x1, x2)):
                total += dot(wf[:, k * chunk : (k + 1) * chunk], ref[...], 1, 0)
            out[...] = (total + dot(wf[:, columns:], sm[...], 1, 0)).astype(bf16)

        return pl.pallas_call(
            body,
            grid=(width // 512,),
            in_specs=[
                spec((512, inner), lambda i: (i, 0)),
                spec((512, full.shape[1]), lambda i: (i, 0)),
                spec((inner, length), lambda i: (0, g)),
            ]
            + [spec((chunk, length), lambda i: (0, 0))] * steps
            + [spec((small.shape[0], length), lambda i: (0, 0))],
            out_specs=spec((512, length), lambda i: (i, 0)),
            out_shape=jax.ShapeDtypeStruct((width, length), bf16),
            compiler_params=params(),
            cost_estimate=cost(13),
            name="dots",
        )(gate_full, full, grad_gate_in, *gx, small)

    gxs = [[None] * steps for _ in range(groups)]
    sums = [()] * groups
    backs = [[None] * steps for _ in range(groups)]
    states_, smalls, normed_grads, step_sums = [], [], [], []
    plan = {0: [out_sum, gate_sum], 1: [out_sum], 2: [gate_sum], 3: [out_sum], 4: [gate_sum], 5: [out_sum]}
    latest, waits = {}, []
    for g in range(groups):
        for i in range(steps):
            k = g * steps + i
            for gradient in plan.get(k, ()):
                latest[gradient] = next(gradient)
                waits.append(latest[gradient])
            backs[g][i] = out = back(g, i, fence(skip_rows, *waits), sums[g])
            waits = []
            gxs[g][i], sums[g] = out[0], (out[6], out[7])
        states_.append(state_back(g))
        for i in range(steps):
            gxs[g][i] = with_returned(gxs[g][i], returned(backs[g][i][1]))
        block = slice(g * length, (g + 1) * length)
        grad_tot = jnp.concatenate([backs[g][i][4] for i in range(steps)], axis=0)
        grad_stride = jnp.concatenate([backs[g][i][3] for i in range(steps)], axis=0)
        grad_rate = jnp.einsum(
            "hkt,st->hks", grad_tot.reshape(heads, blocks, BLOCK), upto, precision=exact
        ).reshape(heads, length)
        grad_pre_step = (grad_stride - grad_rate * pace) * jax.nn.sigmoid(biased[:, block])
        step_sums.append(
            (jnp.sum(grad_pre_step, axis=1), jnp.sum(grad_rate * rate[:, block], axis=1))
        )
        grad_state = states_[g][0]
        grad_state = grad_state + jnp.pad(returned(states_[g][1]), ((0, 0), (length - 3, 0)))
        grad_step_in = grad_pre_step.astype(bf16).astype(f32)
        smalls.append(
            split(jnp.concatenate([grad_state, grad_step_in, jnp.zeros((pad, length), f32)], axis=0))
        )
        normed_grads.append(dots_of(g, gxs[g], smalls[g][0]))
    normed_came = [shifted(a, "head", 1) for a in normed_grads]
    grad_step_bias = sum(a for a, _ in step_sums)
    grad_decay_log = sum(a for _, a in step_sums)
    grad_skip = sum(
        jnp.concatenate([jnp.sum(backs[g][i][5], axis=1) for i in range(steps)]) for g in range(groups)
    )
    def last_of(gradient):
        for value in gradient:
            latest[gradient] = value
        return latest[gradient]

    out_share = spread_rows([last_of(out_sum)]).T
    gate_share = spread_rows([last_of(gate_sum)])
    parts = [jnp.concatenate([gxs[g][i] for g in range(groups)], axis=1) for i in range(steps)]
    totals = [reduction(normed_theirs, normed_mine, part) for part in parts]
    small_high, small_low = (jnp.concatenate(terms, axis=1) for terms in zip(*smalls))
    totals.append(reduction(normed_theirs, normed_mine, small_high, small_low, f32))
    for _ in range(3):
        for gradient in totals:
            next(gradient)
    totals = [next(gradient) for gradient in totals]
    small_total = totals.pop()
    other = shifted(small_total[:, : 2 * n], "head", 1)
    small_total = jnp.concatenate([small_total[:, : 2 * n] + other, small_total[:, 2 * n :]], axis=1)
    small_share = spread_rows([small_total])
    input_share = spread_rows(totals)
    state_share = small_share[:, : 2 * n]
    step_share = small_share[:, 2 * n : small]

    def finish(g, before):
        held = 0 if before is None else 1

        def body(*refs):
            own, came, tok, cot, gain = refs[:5]
            out, sums = refs[5 + held :]
            total = jnp.transpose(own[...].astype(f32) + came[...].astype(f32))
            plain = tok[...].astype(f32)
            factor = inverse_root(jnp.mean(plain * plain, axis=1, keepdims=True) + 1e-05)
            spread = total * gain[...]
            inward = jnp.sum(spread * plain, axis=1, keepdims=True) / width
            out[...] = (
                cot[...].astype(f32) + factor * spread - plain * (factor * factor * factor) * inward
            ).astype(bf16)
            part = jnp.sum(total * plain * factor, axis=0, keepdims=True)

            @pl.when(pl.program_id(0) == 0)
            def _():
                sums[...] = jnp.zeros_like(sums)

            sums[0:1, :] += part

        many = length // LANES
        return pl.pallas_call(
            body,
            grid=(many,),
            in_specs=[
                spec((width, LANES), lambda i: (0, i)),
                spec((width, LANES), lambda i: (0, i)),
                spec((LANES, width), lambda i: (g * many + i, 0)),
                spec((LANES, width), lambda i: (g * many + i, 0)),
                spec((1, width), lambda i: (0, 0)),
            ]
            + [pl.BlockSpec(memory_space=pl.ANY)] * held,
            out_specs=[
                spec((LANES, width), lambda i: (g * many + i, 0)),
                spec((8, width), lambda i: (0, 0)),
            ],
            out_shape=[
                jax.ShapeDtypeStruct((count, width), bf16),
                jax.ShapeDtypeStruct((8, width), f32),
            ],
            input_output_aliases={5: 0} if held else {},
            compiler_params=params(),
            cost_estimate=cost(4),
            name="finish",
        )(
            normed_grads[g], normed_came[g], tokens.reshape(count, width), upstream, norm_gain[None],
            *([] if before is None else [before]),
        )

    grad_tokens, grad_norm_gain = None, 0.0
    for g in range(groups):
        grad_tokens, part = finish(g, grad_tokens)
        grad_norm_gain = grad_norm_gain + part[0]
    grad_tokens = grad_tokens.reshape(groups, length, width)

    grad_taps = sum(
        jnp.concatenate([backs[g][i][2][:, :5] for i in range(steps)], axis=0) for g in range(groups)
    )
    grad_taps_state = sum(states_[g][2] for g in range(groups))[:, :5]
    state_sum = grad_taps_state.T.reshape(-1)
    state_sum = state_sum + shifted(state_sum, "head", 1)
    vector = jnp.concatenate(
        [grad_taps.T.reshape(-1), state_sum, grad_step_bias, grad_decay_log, grad_skip, grad_inner_gain]
    )
    vector = all_sum(vector, "dp", "seq")
    grad_norm_gain = all_sum(grad_norm_gain, "dp", "seq")
    taps_sum = vector[: 5 * inner].reshape(5, inner)
    state_sum = vector[5 * inner : 5 * inner + 10 * n].reshape(5, 2 * n)
    rest = vector[5 * inner + 10 * n :]
    return (
        block_out,
        grad_tokens,
        grad_norm_gain,
        gate_share,
        input_share,
        state_share,
        step_share,
        taps_sum[:4],
        taps_sum[4],
        state_sum[:4],
        state_sum[4],
        rest[:heads],
        rest[heads : 2 * heads],
        rest[2 * heads : 3 * heads],
        rest[3 * heads :],
        out_share,
    )


def solution(mesh):
    in_specs = (
        P("dp", "seq", None),
        P("dp", "seq", None),
        P("dp", "seq"),
        P(),
        P("seq", "head"),
        P("seq", "head"),
        P("seq", None),
        P("seq", "head"),
        P(None, "head"),
        P("head"),
        P(),
        P(),
        P("head"),
        P("head"),
        P("head"),
        P("head"),
        P("head", "seq"),
    )
    out_specs = (
        P("dp", "seq", None),
        P("dp", "seq", None),
        P(),
        P("seq", "head"),
        P("seq", "head"),
        P("seq", None),
        P("seq", "head"),
        P(None, "head"),
        P("head"),
        P(),
        P(),
        P("head"),
        P("head"),
        P("head"),
        P("head"),
        P("head", "seq"),
    )
    return jax.shard_map(
        per_device, mesh=mesh, in_specs=in_specs, out_specs=out_specs, check_vma=False
    )
```

```python
import functools

import jax
import jax.numpy as jnp
from jax import lax
from jax.experimental import pallas as pl
from jax.experimental.pallas import tpu as pltpu
from jax.sharding import PartitionSpec as P


BLOCK = 128
GROUP = 8
LANES = 128
MESH = pl.DeviceIdType.MESH
FAR = -1e30
exact = lax.Precision.HIGHEST
f32 = jnp.float32
bf16 = jnp.bfloat16


def cost(us):
    return pl.CostEstimate(flops=int(us * 1.1e9), bytes_accessed=int(us * 3.0e6), transcendentals=0)


def inverse_root(v):
    r = lax.rsqrt(v)
    return r * (1.5 - 0.5 * v * r * r)


def split(x):
    high = x.astype(bf16)
    return high, (x - high.astype(f32)).astype(bf16)


def dots(a, b, ca, cb):
    return dot(a[0], b[0], ca, cb) + (dot(a[1], b[0], ca, cb) + dot(a[0], b[1], ca, cb))


def pair(ref):
    return ref[0], ref[1]


def maps(bc, lanes):
    n = bc.shape[0] // 4
    return (
        (bc[0:n, lanes], bc[2 * n : 3 * n, lanes]),
        (bc[n : 2 * n, lanes], bc[3 * n : 4 * n, lanes]),
    )


def dot(a, b, ca, cb):
    return lax.dot_general(a, b, (((ca,), (cb,)), ((), ())), preferred_element_type=f32)


def shifted(a, axis, distance):
    n = lax.axis_size(axis)
    return lax.ppermute(a, axis, [(i, (i + distance) % n) for i in range(n)])


def from_behind(a, axis, distance):
    devices = range(lax.axis_size(axis))
    return lax.ppermute(a, axis, [(i, i + distance) for i in devices if i + distance in devices])


def core_swap(a):
    return lax.ppermute(a, "dp", [(i, i ^ 1) for i in range(lax.axis_size("dp"))])


def y_shift(a, distance):
    n = lax.axis_size("dp")
    m = n // 2
    return lax.ppermute(
        a, "dp", [(i, ((i // 2 + distance) % m) * 2 + i % 2) for i in range(n)]
    )


def pick(a, index, axis=0):
    return lax.dynamic_index_in_dim(a, index, axis, False)


def assemble(sources, pieces, shape):
    lead = len(shape) - 2

    def body(*refs):
        where, ins, out = refs[0], refs[1:-1], refs[-1]
        for i in range(len(pieces)):
            at = tuple(where[i * lead + k] for k in range(lead))
            column = sources[i][1]
            out[at + (slice(None), slice(column, column + ins[i].shape[1]))] = ins[i][...]

    table = [jnp.asarray(v, jnp.int32) for source in sources for v in source[0]]
    return pl.pallas_call(
        body,
        out_shape=jax.ShapeDtypeStruct(shape, pieces[0].dtype),
        in_specs=[pl.BlockSpec(memory_space=pltpu.SMEM)]
        + [pl.BlockSpec(memory_space=pltpu.VMEM)] * len(pieces),
        out_specs=pl.BlockSpec(memory_space=pltpu.VMEM),
        compiler_params=pltpu.CompilerParams(vmem_limit_bytes=40 << 20),
        cost_estimate=cost(3.0),
        name="assemble",
    )(jnp.stack(table), *pieces)


def gather_kernel(nz, ny, many, *refs):
    shards, (tokens, tail, cotangent, gain) = refs[:many], refs[many : many + 4]
    fulls = refs[many + 4 : 2 * many + 4]
    ext, up, normed_half, up_half, own, z_send, z_recv, y_send, y_recv, c_send, c_recv = refs[2 * many + 4 :]
    z, d = lax.axis_index("seq"), lax.axis_index("dp")
    y, core = d // 2, lax.rem(d, 2)

    def along_z(hop):
        return {"seq": lax.rem(z + hop, nz)}

    def along_y(step):
        return {"dp": lax.rem(y + step, ny) * 2 + core}

    other = {"dp": y * 2 + 1 - core}
    peers = [along_z(h) for h in range(1, nz)] + [along_y(s) for s in range(1, ny)] + [other]
    barrier = pltpu.get_barrier_semaphore()
    for peer in peers:
        pl.semaphore_signal(barrier, inc=1, device_id=peer, device_id_type=MESH)
    pl.semaphore_wait(barrier, len(peers))

    def copy(src, dst, send, recv, peer):
        return pltpu.make_async_remote_copy(
            src_ref=src, dst_ref=dst, send_sem=send, recv_sem=recv, device_id=peer, device_id_type=MESH
        )

    def z_copy(p, hop):
        return copy(
            shards[p].at[core, y], fulls[p].at[z, core, y], z_send.at[p, hop], z_recv.at[p, hop], along_z(hop)
        )

    def place(p, hop, row):
        return fulls[p].at[lax.rem(z + nz - hop, nz), core, row]

    def y_copy(p, hop, step):
        at = place(p, hop, y)
        return copy(at, at, y_send.at[p, hop, step], y_recv.at[p, hop, step], along_y(step))

    def c_copy(p, hop, step):
        at = place(p, hop, lax.rem(y + ny - step, ny))
        return copy(at, at, c_send.at[p, hop, step], c_recv.at[p, hop, step], other)

    hops = range(1, nz)
    for p in range(many):
        for hop in hops:
            z_copy(p, hop).start()
    for p in range(many):
        pltpu.make_async_copy(shards[p], fulls[p].at[z], own.at[p]).start()

    width = tokens.shape[1]
    blocks = tokens.shape[0] // LANES
    part = width // (2 * nz)

    def norm(rows):
        plain = rows.astype(f32)
        factor = inverse_root(jnp.mean(plain * plain, axis=1, keepdims=True) + 1e-05)
        return (plain * factor * gain[...]).astype(bf16)

    def prepare(i, _):
        at = pl.ds(pl.multiple_of(i * LANES, LANES), LANES)
        for value, whole, half in ((norm(tokens[at, :]), ext, normed_half), (cotangent[at, :], up, up_half)):
            turned = jnp.transpose(value)
            whole[:, at] = turned
            for block in range(2 * nz):
                side = lax.rem(core + block, 2)
                half[side, block // 2 * part : (block // 2 + 1) * part, at] = turned[
                    block * part : (block + 1) * part, :
                ]
        return 0

    lax.fori_loop(0, blocks, prepare, 0)

    def prepare_tail(i, _):
        at = pl.ds(pl.multiple_of(i * LANES, LANES), LANES)
        to = pl.ds(pl.multiple_of((blocks + i) * LANES, LANES), LANES)
        ext[:, to] = jnp.transpose(norm(tail[at, :]))
        return 0

    lax.fori_loop(0, tail.shape[0] // LANES, prepare_tail, 0)
    for p in range(many):
        for hop in hops:
            z_copy(p, hop).wait_recv()
            for step in range(1, ny):
                y_copy(p, hop, step).start()
            c_copy(p, hop, 0).start()
        for hop in hops:
            for step in range(1, ny):
                y_copy(p, hop, step).wait_recv()
                c_copy(p, hop, step).start()
    for p in range(many):
        pltpu.make_async_copy(shards[p], fulls[p].at[z], own.at[p]).wait()
        for hop in hops:
            z_copy(p, hop).wait_send()
            for step in range(1, ny):
                y_copy(p, hop, step).wait_send()
            for step in range(ny):
                c_copy(p, hop, step).wait()


def begin(shards, tokens, tail, cotangent, gain):
    nz, nd = lax.axis_size("seq"), lax.axis_size("dp")
    ny = nd // 2
    many = len(shards)
    split = [a.reshape(2, ny, a.shape[0] // nd, a.shape[1]) for a in shards]
    sems = [(many,), (many, nz), (many, nz), (many, nz, ny), (many, nz, ny), (many, nz, ny), (many, nz, ny)]
    count, width = tokens.shape
    vmem = pl.BlockSpec(memory_space=pltpu.VMEM)
    outs = pl.pallas_call(
        functools.partial(gather_kernel, nz, ny, many),
        out_shape=[jax.ShapeDtypeStruct((nz,) + a.shape, a.dtype) for a in split]
        + [
            jax.ShapeDtypeStruct((width, count + tail.shape[0]), bf16),
            jax.ShapeDtypeStruct((width, count), bf16),
            jax.ShapeDtypeStruct((2, width // 2, count), bf16),
            jax.ShapeDtypeStruct((2, width // 2, count), bf16),
        ],
        in_specs=[vmem] * (many + 4),
        out_specs=[pl.BlockSpec(memory_space=pl.ANY)] * many + [vmem] * 4,
        scratch_shapes=[pltpu.SemaphoreType.DMA(shape) for shape in sems],
        compiler_params=pltpu.CompilerParams(
            collective_id=0, has_side_effects=True, vmem_limit_bytes=56 << 20
        ),
        name="gather",
    )(*split, tokens, tail, cotangent, gain)
    fulls = [full.reshape(nz * a.shape[0], a.shape[1]) for full, a in zip(outs, shards)]
    return fulls, outs[many:]


def all_sum(a, *axes):
    for axis in axes:
        n = lax.axis_size(axis)
        bit = 1
        while bit < n:
            a = a + lax.ppermute(a, axis, [(i, i ^ bit) for i in range(n)])
            bit *= 2
    return a


def reduction(theirs, mine, right, low=None, kind=bf16):
    nz, nd = lax.axis_size("seq"), lax.axis_size("dp")
    ny = nd // 2
    z, d = lax.axis_index("seq"), lax.axis_index("dp")
    y = d // 2

    def product(left):
        full = dot(left, right, 1, 1)
        return full if low is None else full + dot(left, low, 1, 1)

    first = product(theirs)
    yield first
    summed = product(mine) + core_swap(first)
    summed = summed.reshape(nz, ny, -1, summed.shape[1])
    sends = [pick(summed, (y + step) % ny, 1).astype(kind) for step in range(1, ny)]
    own = pick(summed, y, 1)
    yield sends
    for step in range(1, ny):
        own = own + y_shift(sends[step - 1], step).astype(f32)
    sends = [pick(own, (z + step) % nz).astype(kind) for step in range(1, nz)]
    total = pick(own, z)
    yield sends
    for step in range(1, nz):
        total = total + shifted(sends[step - 1], "seq", step).astype(f32)
    yield total


def fence(value, *others):
    return lax.optimization_barrier((value, others))[0]


def spread_rows(totals):
    nd = lax.axis_size("dp")
    ny = nd // 2
    d = lax.axis_index("dp")
    y, core = d // 2, d % 2
    pieces, sources, column = [], [], 0
    for total in totals:
        held = [(y, total)]
        for step in range(1, ny):
            held.append(((y - step) % ny, y_shift(total, step)))
        for row, piece in held:
            pieces.append(piece)
            sources.append(((core, row), column))
            pieces.append(core_swap(piece))
            sources.append(((1 - core, row), column))
        column += total.shape[1]
    r = totals[0].shape[0]
    return assemble(sources, pieces, (2, ny, r, column)).reshape(nd * r, column)


def chain_states(value, fading, reverse):
    n = lax.axis_size("seq")
    came = jnp.zeros(value.shape, f32)
    for hop in range(1, n):
        pair_of = (n - hop, n - 1 - hop) if reverse else (hop - 1, hop)
        send = value + fading * came if hop > 1 else value
        came = came + lax.ppermute(send, "seq", [pair_of])
    return came


def row_iota(n):
    return lax.broadcasted_iota(jnp.int32, (1, n), 1)


def allowed_rows(starts, length):
    places = row_iota(length)
    return [None] + [(starts <= places - delay).astype(f32) for delay in (1, 2, 3)]


def conv_rows(x, halo, taps, allowed):
    x = x.astype(f32)
    joined = jnp.concatenate([halo.astype(f32), x], axis=1)
    pre = taps[:, 4:5] + taps[:, 3:4] * x
    moved = [x]
    for delay in (1, 2, 3):
        m = pltpu.roll(joined, delay, 1)[:, LANES:] * allowed[delay]
        moved.append(m)
        pre = pre + taps[:, 3 - delay : 4 - delay] * m
    return pre, moved


def conv_back(grad, moved, taps, allowed):
    rows, length = grad.shape
    lane = lax.broadcasted_iota(jnp.int32, (rows, LANES), 1)
    joined = jnp.zeros((rows, LANES + length), f32)
    sums = jnp.where(lane == 4, jnp.sum(grad, axis=1, keepdims=True), 0.0)
    blank = jnp.zeros((rows, LANES), f32)
    for delay in range(4):
        part = jnp.sum(grad * moved[delay], axis=1, keepdims=True)
        sums = jnp.where(lane == 3 - delay, part, sums)
        v = taps[:, 3 - delay : 4 - delay] * grad
        if delay:
            v = v * allowed[delay]
        v = jnp.concatenate([blank, v], axis=1)
        if delay:
            v = pltpu.roll(v, LANES + length - delay, 1)
        joined = joined + v
    return joined, sums


def block_masks(starts, c):
    s = lax.broadcasted_iota(jnp.int32, (BLOCK, BLOCK), 0) + c * BLOCK
    t = lax.broadcasted_iota(jnp.int32, (BLOCK, BLOCK), 1) + c * BLOCK
    row = row_iota(BLOCK) + c * BLOCK
    last = starts[:, BLOCK - 1 : BLOCK]
    visible = jnp.where((starts <= s) & (s <= t), 0.0, FAR)
    carried = jnp.where(starts < c * BLOCK, 0.0, FAR)
    tail = jnp.where(row >= last, 0.0, FAR)
    carried_last = jnp.where(last < c * BLOCK, 0.0, FAR)
    return visible, carried, tail, carried_last


def column(row):
    return jnp.transpose(jnp.broadcast_to(row, (BLOCK, BLOCK)))


def local_kernel(x, hx, st, hst, taps, taps_st, starts, tot, stride, skip, y, end, bc, xs, state, inter, weighted):
    length = x.shape[1]
    rows = x.shape[0] // GROUP
    allowed = allowed_rows(starts[...], length)

    @pl.when(pl.program_id(0) == 0)
    def _():
        def one(i, _):
            at = pl.ds(pl.multiple_of(i * 64, 64), 64)
            pre, _m = conv_rows(st[at, :], hst[at, :], taps_st[at, :], allowed)
            high, low = split(pre * jax.nn.sigmoid(pre))
            bc[at, :] = high
            bc[pl.ds(pl.multiple_of(st.shape[0] + i * 64, 64), 64), :] = low
            return 0

        lax.fori_loop(0, st.shape[0] // 64, one, 0)

    def conv(i, _):
        at = pl.ds(pl.multiple_of(i * rows, rows), rows)
        pre, _m = conv_rows(x[at, :], hx[at, :], taps[at, :], allowed)
        xs[at, :] = pre * jax.nn.sigmoid(pre)
        return 0

    lax.fori_loop(0, GROUP, conv, 0)
    state[...] = jnp.zeros_like(state)

    def block(c, _):
        lanes = pl.ds(pl.multiple_of(c * BLOCK, BLOCK), BLOCK)
        write, read = maps(bc, lanes)
        cross = dots(write, read, 0, 0)
        visible, carried, tail, carried_last = block_masks(starts[:, lanes], c)
        inter[...] = dots(split(state[...]), read, 1, 0)
        for h in range(GROUP):
            at = slice(h * rows, (h + 1) * rows)
            total = tot[h : h + 1, lanes]
            ending = total[:, BLOCK - 1 : BLOCK]
            fade = jnp.exp(total - column(total) + visible)
            mixing = (cross * fade).astype(bf16)
            feed = xs[at, lanes]
            scaled = feed * stride[h : h + 1, lanes]
            y[at, lanes] = (
                dot(scaled.astype(bf16), mixing, 1, 0)
                + inter[at, :] * jnp.exp(total + carried)
                + skip[h : h + 1, :] * feed
            )
            for k, term in enumerate(split(scaled * jnp.exp(ending - total + tail))):
                weighted[k, at, :] = term
            state[at, :] = state[at, :] * jnp.exp(ending + carried_last)
        state[...] += dots(pair(weighted), write, 1, 1)
        return 0

    lax.fori_loop(0, length // BLOCK, block, 0)
    end[...] = state[...]


def join_kernel(y, entering, read, read_low, edev, gate, grad_inner, taps, mixer, sums, inter):
    rows = y.shape[0] // GROUP

    @pl.when(pl.program_id(0) == 0)
    def _():
        sums[...] = jnp.zeros_like(sums)

    inter[...] = dots(split(entering[...]), (read[...], read_low[...]), 1, 0)

    def one(h, total):
        at = pl.ds(pl.multiple_of(h * rows, rows), rows)
        m = y[at, :] + inter[at, :] * edev[pl.ds(h, 1), :]
        mixer[at, :] = m
        g = gate[at, :]
        gated = m * (g * jax.nn.sigmoid(g))
        square = jnp.sum(gated * gated, axis=0, keepdims=True)
        product = jnp.sum(grad_inner[at, :] * taps[at, 5:6] * gated, axis=0, keepdims=True)
        return total[0] + square, total[1] + product

    zero = jnp.zeros((1, y.shape[1]), f32)
    square, product = lax.fori_loop(0, GROUP, one, (zero, zero))
    sums[0:1, :] += square
    sums[1:2, :] += product


def gate_kernel(inner_total, aliased, *refs):
    mixer, gate, grad_inner, own, came, edev, read, read_low, taps = refs[:9]
    inner_out, grad_mixer, grad_gate, grad_entering, grad_gain, faded = refs[9 + 2 * aliased :]
    rows = mixer.shape[0] // GROUP
    summed = own[0:2, :] + came[0:2, :]
    scale = inverse_root(summed[0:1, :] / inner_total + 1e-05)
    back = scale * scale * scale * (summed[1:2, :] / inner_total)

    def one(h, _):
        at = pl.ds(pl.multiple_of(h * rows, rows), rows)
        m, g, gi = mixer[at, :], gate[at, :], grad_inner[at, :]
        sigma = jax.nn.sigmoid(g)
        opened = g * sigma
        gated = m * opened
        gain = taps[at, 5:6]
        normal = gated * scale
        inner_out[at, :] = (normal * gain).astype(bf16)
        grad_gain[at, :] = jnp.broadcast_to(jnp.sum(gi * normal, axis=1, keepdims=True), (rows, LANES))
        grad_gated = scale * (gi * gain) - gated * back
        gm = grad_gated * opened
        grad_mixer[at, :] = gm
        grad_gate[at, :] = (grad_gated * m * sigma * (1.0 + g * (1.0 - sigma))).astype(bf16)
        for k, term in enumerate(split(gm * edev[pl.ds(h, 1), :])):
            faded[k, at, :] = term
        return 0

    lax.fori_loop(0, GROUP, one, 0)
    grad_entering[...] = dots(pair(faded), (read[...], read_low[...]), 1, 1)


def back_kernel(first, last, *refs):
    (x, hx, taps, starts, tot, stride, skip, grad_mixer, entering, later, bc) = refs[:11]
    if not first:
        gbc_before, gcross_before = refs[11:13]
    at_out = 11 if first else 13
    (gx, ghalo, gtaps, gstride, gtot, gskip, gbc, gcross) = refs[at_out : at_out + 8]
    xs, slope, gfeed, states, state, gstate, cross_from, cross_to, weighted, faded = refs[at_out + 8 :]
    length = x.shape[1]
    rows = x.shape[0] // GROUP
    n = bc.shape[0] // 4
    blocks = length // BLOCK
    allowed = allowed_rows(starts[...], length)
    if first:
        gbc[...] = jnp.zeros_like(gbc)
        gcross[...] = jnp.zeros_like(gcross)
    else:
        gbc[...] = gbc_before[...]
        gcross[...] = gcross_before[...]

    def conv(i, _):
        at = pl.ds(pl.multiple_of(i * rows, rows), rows)
        pre, _m = conv_rows(x[at, :], hx[at, :], taps[at, :], allowed)
        s = jax.nn.sigmoid(pre)
        xs[at, :] = pre * s
        slope[at, :] = s * (1.0 + pre * (1.0 - s))
        return 0

    lax.fori_loop(0, GROUP, conv, 0)
    state[...] = entering[...].astype(f32)

    def ahead(c, _):
        lanes = pl.ds(pl.multiple_of(c * BLOCK, BLOCK), BLOCK)
        for k, term in enumerate(split(state[...])):
            states[k, c] = term
        _v, _c, tail, carried_last = block_masks(starts[:, lanes], c)
        for h in range(GROUP):
            at = slice(h * rows, (h + 1) * rows)
            total = tot[h : h + 1, lanes]
            ending = total[:, BLOCK - 1 : BLOCK]
            scaled = xs[at, lanes] * stride[h : h + 1, lanes]
            for k, term in enumerate(split(scaled * jnp.exp(ending - total + tail))):
                weighted[k, at, :] = term
            state[at, :] = state[at, :] * jnp.exp(ending + carried_last)
        state[...] += dots(pair(weighted), maps(bc, lanes)[0], 1, 1)
        return 0

    lax.fori_loop(0, blocks - 1, ahead, 0)
    for k, term in enumerate(split(state[...])):
        states[k, blocks - 1] = term
    gstate[...] = later[...].astype(f32)
    ones = jnp.ones((8, BLOCK), bf16)
    lastlane = row_iota(BLOCK) == BLOCK - 1

    def block(i, _):
        c = blocks - 1 - i
        lanes = pl.ds(pl.multiple_of(c * BLOCK, BLOCK), BLOCK)
        write, read = maps(bc, lanes)
        cross = dots(write, read, 0, 0)
        visible, carried, tail, carried_last = block_masks(starts[:, lanes], c)
        before = (states[0, c], states[1, c])
        after = split(gstate[...])
        cross_from[...] = dot(before[0], read[0], 1, 0)
        cross_to[...] = dot(after[0], write[0], 1, 0)
        mixed = jnp.zeros((BLOCK, BLOCK), f32)
        for h in range(GROUP):
            at = slice(h * rows, (h + 1) * rows)
            total = tot[h : h + 1, lanes]
            ending = total[:, BLOCK - 1 : BLOCK]
            fade = jnp.exp(total - column(total) + visible)
            enter = jnp.exp(total + carried)
            weight = jnp.exp(ending - total + tail)
            decay = jnp.exp(ending + carried_last)
            feed = xs[at, lanes]
            pace = stride[h : h + 1, lanes]
            scaled = feed * pace
            gm = grad_mixer[at, lanes]
            gms = split(gm)
            outer = dots(split(scaled), gms, 0, 0) * fade
            mixed = mixed + outer
            pairs = (outer * cross).astype(bf16)
            mixing = (cross * fade).astype(bf16)
            leaving = cross_to[at, :] * weight
            reach = dot(gms[0], mixing, 1, 1) + leaving
            gfeed[at, lanes] = pace * reach + skip[h : h + 1, :] * gm
            gstride[h : h + 1, lanes] = jnp.sum(feed * reach, axis=0, keepdims=True)
            left = jnp.sum(scaled * leaving, axis=0, keepdims=True)
            came = jnp.sum(gm * cross_from[at, :], axis=0, keepdims=True) * enter
            into = jnp.sum(pairs.astype(f32), axis=0, keepdims=True)
            out = dot(ones, pairs, 1, 1)[0:1, :]
            held = gstate[at, :]
            flux = jnp.sum(
                jnp.sum(before[0][at, :].astype(f32) * held, axis=0, keepdims=True), axis=1, keepdims=True
            )
            final = jnp.sum(left, axis=1, keepdims=True) + flux * decay
            gtot[h : h + 1, lanes] = into - out + came - left + jnp.where(lastlane, final, 0.0)
            dskip = jnp.sum(gm * feed, axis=0, keepdims=True)
            gskip[h : h + 1, :] = jnp.where(i == 0, dskip, gskip[h : h + 1, :] + dskip)
            for k, term in enumerate(split(gm * enter)):
                faded[k, at, :] = term
            for k, term in enumerate(split(scaled * weight)):
                weighted[k, at, :] = term
            gstate[at, :] = held * decay
        gcross[c] += mixed
        gbc[n : 2 * n, lanes] += dots(before, pair(faded), 0, 0)
        gbc[0:n, lanes] += dots(after, pair(weighted), 0, 0)
        gstate[...] += dots(pair(faded), read, 1, 1)
        return 0

    lax.fori_loop(0, blocks, block, 0)

    def conv_grad(i, _):
        at = pl.ds(pl.multiple_of(i * rows, rows), rows)
        _p, moved = conv_rows(x[at, :], hx[at, :], taps[at, :], allowed)
        joined, sums = conv_back(gfeed[at, :] * slope[at, :], moved, taps[at, :], allowed)
        gx[at, :] = joined[:, LANES:].astype(bf16)
        ghalo[at, :] = joined[:, :LANES].astype(bf16)
        gtaps[at, :] = sums
        return 0

    lax.fori_loop(0, GROUP, conv_grad, 0)

    if last:

        def one(c, _):
            lanes = pl.ds(pl.multiple_of(c * BLOCK, BLOCK), BLOCK)
            write, read = maps(bc, lanes)
            terms = split(gcross[c])
            gbc[n : 2 * n, lanes] += dots(write, terms, 1, 0)
            gbc[0:n, lanes] += dots(read, terms, 1, 1)
            return 0

        lax.fori_loop(0, blocks, one, 0)


def state_back_kernel(st, hst, taps, starts, gbc, gst, ghalo, gtaps):
    length = st.shape[1]
    allowed = allowed_rows(starts[...], length)

    def one(i, _):
        at = pl.ds(pl.multiple_of(i * 64, 64), 64)
        pre, moved = conv_rows(st[at, :], hst[at, :], taps[at, :], allowed)
        s = jax.nn.sigmoid(pre)
        grad = gbc[at, :] * (s * (1.0 + pre * (1.0 - s)))
        joined, sums = conv_back(grad, moved, taps[at, :], allowed)
        gst[at, :] = joined[:, LANES:]
        ghalo[at, :] = joined[:, :LANES]
        gtaps[at, :] = sums
        return 0

    lax.fori_loop(0, st.shape[0] // 64, one, 0)


def params():
    return pltpu.CompilerParams(vmem_limit_bytes=48 << 20)


def per_device(
    tokens,
    cotangent,
    doc_start,
    norm_gain,
    gate_proj,
    input_proj,
    state_proj,
    step_proj,
    inner_kernel,
    inner_shift,
    state_kernel,
    state_shift,
    step_bias,
    decay_log,
    skip_gain,
    inner_gain,
    out_proj,
):
    groups, length, width = tokens.shape
    count = groups * length
    heads = step_bias.shape[0]
    inner = inner_gain.shape[0]
    headsize = inner // heads
    n = state_kernel.shape[1] // 2
    chunk = GROUP * headsize
    steps = heads // GROUP
    blocks = length // BLOCK
    inner_total = inner * lax.axis_size("head")

    small = 2 * n + heads
    pad = -small % LANES
    packed = jnp.concatenate(
        [input_proj, state_proj, step_proj, jnp.zeros((input_proj.shape[0], pad), bf16)], axis=1
    )
    tail = from_behind(tokens[:, length - 3 :, :], "seq", 1)
    tail = jnp.pad(tail, ((0, 0), (LANES - 3, 0), (0, 0))).reshape(groups * LANES, width)
    upstream = cotangent.reshape(count, width)
    (full, gate_full, out_full), (ext, up_t, normed_half, up_half) = begin(
        [packed, gate_proj, out_proj.T], tokens.reshape(count, width), tail, upstream, norm_gain[None]
    )
    normed_mine, normed_theirs = normed_half[0], normed_half[1]
    up_mine, up_theirs = up_half[0], up_half[1]
    plain = tokens.reshape(count, width).astype(f32)

    starts = doc_start - lax.axis_index("seq") * length
    starts_row = starts.reshape(1, count)
    taps = jnp.concatenate(
        [
            jnp.concatenate([inner_kernel, state_kernel], axis=1),
            jnp.concatenate([inner_shift, state_shift])[None],
            jnp.concatenate([inner_gain, jnp.zeros((2 * n,), f32)])[None],
            jnp.zeros((2, inner + 2 * n), f32),
        ],
        axis=0,
    ).T
    skip_rows = jnp.broadcast_to(skip_gain[:, None], (heads, LANES))

    proj = dot(full[:, : inner + 2 * n], ext, 0, 0).astype(bf16)
    step_in = dot(full[:, inner + 2 * n :], ext[:, :count], 0, 0)[:heads]
    biased = step_in + step_bias[:, None]
    stride = jax.nn.softplus(biased)
    pace = jnp.exp(decay_log)[:, None]
    rate = -stride * pace
    upto = jnp.triu(jnp.ones((BLOCK, BLOCK), f32))
    tot3 = jnp.einsum("hks,st->hkt", rate.reshape(heads, groups * blocks, BLOCK), upto, precision=exact)
    tot = tot3.reshape(heads, count)
    ends = tot3[:, :, BLOCK - 1].reshape(heads, groups, blocks)
    before = jnp.cumsum(ends, axis=2) - ends
    from_start = tot.reshape(heads, groups, blocks, BLOCK) + before[..., None]
    edev = jnp.where((starts < 0)[None], jnp.exp(from_start.reshape(heads, groups, length)), 0.0)
    edev = edev.reshape(heads, count)
    fading = jnp.where(starts[None, :, -1] < 0, jnp.exp(jnp.sum(ends, axis=2)), 0.0)
    fading = jnp.repeat(fading, headsize, axis=0)

    halo_at = count // LANES
    grid = (steps,)

    def spec(shape, where):
        return pl.BlockSpec(shape, where)

    def local(g):
        return pl.pallas_call(
            local_kernel,
            grid=grid,
            in_specs=[
                spec((chunk, length), lambda i: (i, g)),
                spec((chunk, LANES), lambda i: (i, halo_at + g)),
                spec((2 * n, length), lambda i: (inner // (2 * n), g)),
                spec((2 * n, LANES), lambda i: (inner // (2 * n), halo_at + g)),
                spec((chunk, 8), lambda i: (i, 0)),
                spec((2 * n, 8), lambda i: (inner // (2 * n), 0)),
                spec((1, length), lambda i: (0, g)),
                spec((GROUP, length), lambda i: (i, g)),
                spec((GROUP, length), lambda i: (i, g)),
                spec((GROUP, LANES), lambda i: (i, 0)),
            ],
            out_specs=[
                spec((chunk, length), lambda i: (i, 0)),
                spec((chunk, n), lambda i: (i, 0)),
                spec((4 * n, length), lambda i: (0, 0)),
            ],
            out_shape=[
                jax.ShapeDtypeStruct((inner, length), f32),
                jax.ShapeDtypeStruct((inner, n), f32),
                jax.ShapeDtypeStruct((4 * n, length), bf16),
            ],
            scratch_shapes=[
                pltpu.VMEM((chunk, length), f32),
                pltpu.VMEM((chunk, n), f32),
                pltpu.VMEM((chunk, BLOCK), f32),
                pltpu.VMEM((2, chunk, BLOCK), bf16),
            ],
            compiler_params=params(),
            cost_estimate=cost(12.5),
            name="local",
        )(proj, proj, proj, proj, taps, taps, starts_row, tot, stride, skip_rows)

    locals_ = [local(g) for g in range(groups)]
    entering = [chain_states(locals_[g][1], fading[:, g : g + 1], False) for g in range(groups)]
    gate_in = dot(gate_full, ext[:, :count], 0, 0)
    grad_inner = dot(out_full, up_t, 0, 0)

    def join(g):
        return pl.pallas_call(
            join_kernel,
            grid=grid,
            in_specs=[
                spec((chunk, length), lambda i: (i, 0)),
                spec((chunk, n), lambda i: (i, 0)),
                spec((n, length), lambda i: (1, 0)),
                spec((n, length), lambda i: (3, 0)),
                spec((GROUP, length), lambda i: (i, g)),
                spec((chunk, length), lambda i: (i, g)),
                spec((chunk, length), lambda i: (i, g)),
                spec((chunk, 8), lambda i: (i, 0)),
            ],
            out_specs=[
                spec((chunk, length), lambda i: (i, 0)),
                spec((8, length), lambda i: (0, 0)),
            ],
            out_shape=[
                jax.ShapeDtypeStruct((inner, length), f32),
                jax.ShapeDtypeStruct((8, length), f32),
            ],
            scratch_shapes=[pltpu.VMEM((chunk, length), f32)],
            compiler_params=params(),
            cost_estimate=cost(6),
            name="join",
        )(locals_[g][0], entering[g], locals_[g][2], locals_[g][2], edev, gate_in, grad_inner, taps)

    joined = [join(g) for g in range(groups)]
    came = [shifted(joined[g][1], "head", 1) for g in range(groups)]

    def gating(g, carried):
        aliased = len(carried)
        return pl.pallas_call(
            functools.partial(gate_kernel, inner_total, aliased // 2),
            grid=grid,
            in_specs=[
                spec((chunk, length), lambda i: (i, 0)),
                spec((chunk, length), lambda i: (i, g)),
                spec((chunk, length), lambda i: (i, g)),
                spec((8, length), lambda i: (0, 0)),
                spec((8, length), lambda i: (0, 0)),
                spec((GROUP, length), lambda i: (i, g)),
                spec((n, length), lambda i: (1, 0)),
                spec((n, length), lambda i: (3, 0)),
                spec((chunk, 8), lambda i: (i, 0)),
            ]
            + [pl.BlockSpec(memory_space=pl.ANY)] * aliased,
            out_specs=[
                spec((chunk, length), lambda i: (i, g)),
                spec((chunk, length), lambda i: (i, 0)),
                spec((chunk, length), lambda i: (i, g)),
                spec((chunk, n), lambda i: (i, 0)),
                spec((chunk, LANES), lambda i: (i, 0)),
            ],
            out_shape=[
                jax.ShapeDtypeStruct((inner, count), bf16),
                jax.ShapeDtypeStruct((inner, length), f32),
                jax.ShapeDtypeStruct((inner, count), bf16),
                jax.ShapeDtypeStruct((inner, n), f32),
                jax.ShapeDtypeStruct((inner, LANES), f32),
            ],
            scratch_shapes=[pltpu.VMEM((2, chunk, length), bf16)],
            input_output_aliases={9: 0, 10: 2} if aliased else {},
            compiler_params=params(),
            cost_estimate=cost(9),
            name="gating",
        )(joined[g][0], gate_in, grad_inner, joined[g][1], came[g], edev, locals_[g][2], locals_[g][2], taps, *carried)

    gated, carried = [], ()
    for g in range(groups):
        gated.append(gating(g, carried))
        carried = (gated[g][0], gated[g][2])
    inner_out, grad_gate_in = carried
    later = [chain_states(gated[g][3], fading[:, g : g + 1], True) for g in range(groups)]
    grad_inner_gain = sum(gated[g][4][:, 0] for g in range(groups))

    branch = dot(inner_out, out_full, 0, 1).astype(bf16)
    branch_came = shifted(branch, "head", 1)
    block_out = (plain + (branch.astype(f32) + branch_came.astype(f32))).astype(bf16)
    block_out = block_out.reshape(groups, length, width)

    out_sum = reduction(up_theirs, up_mine, inner_out)
    gate_sum = reduction(normed_theirs, normed_mine, grad_gate_in)

    def back(g, i, skip_rows, sums):
        at = lambda *where: (lambda _: where)
        return pl.pallas_call(
            functools.partial(back_kernel, i == 0, i == steps - 1),
            grid=(1,),
            in_specs=[
                spec((chunk, length), at(i, g)),
                spec((chunk, LANES), at(i, halo_at + g)),
                spec((chunk, 8), at(i, 0)),
                spec((1, length), at(0, g)),
                spec((GROUP, length), at(i, g)),
                spec((GROUP, length), at(i, g)),
                spec((GROUP, LANES), at(i, 0)),
                spec((chunk, length), at(i, 0)),
                spec((chunk, n), at(i, 0)),
                spec((chunk, n), at(i, 0)),
                spec((4 * n, length), at(0, 0)),
            ]
            + [spec((2 * n, length), at(0, 0)), spec((blocks, BLOCK, BLOCK), at(0, 0, 0))][: len(sums)],
            out_specs=[
                spec((chunk, length), at(0, 0)),
                spec((chunk, LANES), at(0, 0)),
                spec((chunk, LANES), at(0, 0)),
                spec((GROUP, length), at(0, 0)),
                spec((GROUP, length), at(0, 0)),
                spec((GROUP, LANES), at(0, 0)),
                spec((2 * n, length), at(0, 0)),
                spec((blocks, BLOCK, BLOCK), at(0, 0, 0)),
            ],
            out_shape=[
                jax.ShapeDtypeStruct((chunk, length), bf16),
                jax.ShapeDtypeStruct((chunk, LANES), bf16),
                jax.ShapeDtypeStruct((chunk, LANES), f32),
                jax.ShapeDtypeStruct((GROUP, length), f32),
                jax.ShapeDtypeStruct((GROUP, length), f32),
                jax.ShapeDtypeStruct((GROUP, LANES), f32),
                jax.ShapeDtypeStruct((2 * n, length), f32),
                jax.ShapeDtypeStruct((blocks, BLOCK, BLOCK), f32),
            ],
            scratch_shapes=[
                pltpu.VMEM((chunk, length), f32),
                pltpu.VMEM((chunk, length), f32),
                pltpu.VMEM((chunk, length), f32),
                pltpu.VMEM((2, blocks, chunk, n), bf16),
                pltpu.VMEM((chunk, n), f32),
                pltpu.VMEM((chunk, n), f32),
                pltpu.VMEM((chunk, BLOCK), f32),
                pltpu.VMEM((chunk, BLOCK), f32),
                pltpu.VMEM((2, chunk, BLOCK), bf16),
                pltpu.VMEM((2, chunk, BLOCK), bf16),
            ],
            compiler_params=params(),
            cost_estimate=cost(14),
            name="back",
        )(
            proj, proj, taps, starts_row, tot, stride, skip_rows,
            gated[g][1], entering[g], later[g], locals_[g][2], *sums,
        )

    def state_back(g):
        return pl.pallas_call(
            state_back_kernel,
            grid=(1,),
            in_specs=[
                spec((2 * n, length), lambda i: (inner // (2 * n), g)),
                spec((2 * n, LANES), lambda i: (inner // (2 * n), halo_at + g)),
                spec((2 * n, 8), lambda i: (inner // (2 * n), 0)),
                spec((1, length), lambda i: (0, g)),
                spec((2 * n, length), lambda i: (0, 0)),
            ],
            out_specs=[
                spec((2 * n, length), lambda i: (0, 0)),
                spec((2 * n, LANES), lambda i: (0, 0)),
                spec((2 * n, LANES), lambda i: (0, 0)),
            ],
            out_shape=[
                jax.ShapeDtypeStruct((2 * n, length), f32),
                jax.ShapeDtypeStruct((2 * n, LANES), f32),
                jax.ShapeDtypeStruct((2 * n, LANES), f32),
            ],
            compiler_params=params(),
            cost_estimate=cost(3),
            name="state_back",
        )(proj, proj, taps, starts_row, sums[g][0])

    def returned(halo):
        return from_behind(halo[:, LANES - 3 :], "seq", -1)

    def with_returned(a, came):
        start = length - LANES
        block = lax.slice_in_dim(a, start, start + LANES, axis=1).astype(f32)
        block = block + jnp.pad(came.astype(f32), ((0, 0), (LANES - 3, 0)))
        return lax.dynamic_update_slice_in_dim(a, block.astype(bf16), start, 1)

    def dots_of(g, gx, small):
        def body(wg, wf, gg, x0, x1, x2, sm, out):
            columns = wg.shape[1]
            total = dot(wg[...], gg[...], 1, 0)
            for k, ref in enumerate((x0, x1, x2)):
                total += dot(wf[:, k * chunk : (k + 1) * chunk], ref[...], 1, 0)
            out[...] = (total + dot(wf[:, columns:], sm[...], 1, 0)).astype(bf16)

        return pl.pallas_call(
            body,
            grid=(width // 512,),
            in_specs=[
                spec((512, inner), lambda i: (i, 0)),
                spec((512, full.shape[1]), lambda i: (i, 0)),
                spec((inner, length), lambda i: (0, g)),
            ]
            + [spec((chunk, length), lambda i: (0, 0))] * steps
            + [spec((small.shape[0], length), lambda i: (0, 0))],
            out_specs=spec((512, length), lambda i: (i, 0)),
            out_shape=jax.ShapeDtypeStruct((width, length), bf16),
            compiler_params=params(),
            cost_estimate=cost(13),
            name="dots",
        )(gate_full, full, grad_gate_in, *gx, small)

    gxs = [[None] * steps for _ in range(groups)]
    sums = [()] * groups
    backs = [[None] * steps for _ in range(groups)]
    states_, smalls, normed_grads, step_sums = [], [], [], []
    plan = {0: [out_sum, gate_sum], 1: [out_sum], 2: [gate_sum], 3: [out_sum], 4: [gate_sum], 5: [out_sum]}
    latest, waits = {}, []
    for g in range(groups):
        for i in range(steps):
            k = g * steps + i
            if g and i == 1:
                waits.append(normed_grads[g - 1])
            for gradient in plan.get(k, ()):
                latest[gradient] = next(gradient)
                waits.append(latest[gradient])
            backs[g][i] = out = back(g, i, fence(skip_rows, *waits), sums[g])
            waits = []
            gxs[g][i], sums[g] = out[0], (out[6], out[7])
        states_.append(state_back(g))
        for i in range(steps):
            gxs[g][i] = with_returned(gxs[g][i], returned(backs[g][i][1]))
        block = slice(g * length, (g + 1) * length)
        grad_tot = jnp.concatenate([backs[g][i][4] for i in range(steps)], axis=0)
        grad_stride = jnp.concatenate([backs[g][i][3] for i in range(steps)], axis=0)
        grad_rate = jnp.einsum(
            "hkt,st->hks", grad_tot.reshape(heads, blocks, BLOCK), upto, precision=exact
        ).reshape(heads, length)
        grad_pre_step = (grad_stride - grad_rate * pace) * jax.nn.sigmoid(biased[:, block])
        step_sums.append(
            (jnp.sum(grad_pre_step, axis=1), jnp.sum(grad_rate * rate[:, block], axis=1))
        )
        grad_state = states_[g][0]
        grad_state = grad_state + jnp.pad(returned(states_[g][1]), ((0, 0), (length - 3, 0)))
        grad_step_in = grad_pre_step.astype(bf16).astype(f32)
        smalls.append(
            split(jnp.concatenate([grad_state, grad_step_in, jnp.zeros((pad, length), f32)], axis=0))
        )
        normed_grads.append(dots_of(g, gxs[g], smalls[g][0]))
    normed_came = [shifted(a, "head", 1) for a in normed_grads]
    grad_step_bias = sum(a for a, _ in step_sums)
    grad_decay_log = sum(a for _, a in step_sums)
    grad_skip = sum(
        jnp.concatenate([jnp.sum(backs[g][i][5], axis=1) for i in range(steps)]) for g in range(groups)
    )
    def last_of(gradient):
        for value in gradient:
            latest[gradient] = value
        return latest[gradient]

    out_share = spread_rows([last_of(out_sum)]).T
    gate_share = spread_rows([last_of(gate_sum)])
    parts = [jnp.concatenate([gxs[g][i] for g in range(groups)], axis=1) for i in range(steps)]
    totals = [reduction(normed_theirs, normed_mine, part) for part in parts]
    small_high, small_low = (jnp.concatenate(terms, axis=1) for terms in zip(*smalls))
    totals.append(reduction(normed_theirs, normed_mine, small_high, small_low, f32))
    for _ in range(3):
        for gradient in totals:
            next(gradient)
    totals = [next(gradient) for gradient in totals]
    small_total = totals.pop()
    other = shifted(small_total[:, : 2 * n], "head", 1)
    small_total = jnp.concatenate([small_total[:, : 2 * n] + other, small_total[:, 2 * n :]], axis=1)
    small_share = spread_rows([small_total])
    input_share = spread_rows(totals)
    state_share = small_share[:, : 2 * n]
    step_share = small_share[:, 2 * n : small]

    def finish(g, before):
        held = 0 if before is None else 1

        def body(*refs):
            own, came, tok, cot, gain = refs[:5]
            out, sums = refs[5 + held :]
            total = jnp.transpose(own[...].astype(f32) + came[...].astype(f32))
            plain = tok[...].astype(f32)
            factor = inverse_root(jnp.mean(plain * plain, axis=1, keepdims=True) + 1e-05)
            spread = total * gain[...]
            inward = jnp.sum(spread * plain, axis=1, keepdims=True) / width
            out[...] = (
                cot[...].astype(f32) + factor * spread - plain * (factor * factor * factor) * inward
            ).astype(bf16)
            part = jnp.sum(total * plain * factor, axis=0, keepdims=True)

            @pl.when(pl.program_id(0) == 0)
            def _():
                sums[...] = jnp.zeros_like(sums)

            sums[0:1, :] += part

        many = length // LANES
        return pl.pallas_call(
            body,
            grid=(many,),
            in_specs=[
                spec((width, LANES), lambda i: (0, i)),
                spec((width, LANES), lambda i: (0, i)),
                spec((LANES, width), lambda i: (g * many + i, 0)),
                spec((LANES, width), lambda i: (g * many + i, 0)),
                spec((1, width), lambda i: (0, 0)),
            ]
            + [pl.BlockSpec(memory_space=pl.ANY)] * held,
            out_specs=[
                spec((LANES, width), lambda i: (g * many + i, 0)),
                spec((8, width), lambda i: (0, 0)),
            ],
            out_shape=[
                jax.ShapeDtypeStruct((count, width), bf16),
                jax.ShapeDtypeStruct((8, width), f32),
            ],
            input_output_aliases={5: 0} if held else {},
            compiler_params=params(),
            cost_estimate=cost(4),
            name="finish",
        )(
            normed_grads[g], normed_came[g], tokens.reshape(count, width), upstream, norm_gain[None],
            *([] if before is None else [before]),
        )

    grad_tokens, grad_norm_gain = None, 0.0
    for g in range(groups):
        grad_tokens, part = finish(g, grad_tokens)
        grad_norm_gain = grad_norm_gain + part[0]
    grad_tokens = grad_tokens.reshape(groups, length, width)

    grad_taps = sum(
        jnp.concatenate([backs[g][i][2][:, :5] for i in range(steps)], axis=0) for g in range(groups)
    )
    grad_taps_state = sum(states_[g][2] for g in range(groups))[:, :5]
    state_sum = grad_taps_state.T.reshape(-1)
    state_sum = state_sum + shifted(state_sum, "head", 1)
    vector = jnp.concatenate(
        [grad_taps.T.reshape(-1), state_sum, grad_step_bias, grad_decay_log, grad_skip, grad_inner_gain]
    )
    vector = all_sum(vector, "dp", "seq")
    grad_norm_gain = all_sum(grad_norm_gain, "dp", "seq")
    taps_sum = vector[: 5 * inner].reshape(5, inner)
    state_sum = vector[5 * inner : 5 * inner + 10 * n].reshape(5, 2 * n)
    rest = vector[5 * inner + 10 * n :]
    return (
        block_out,
        grad_tokens,
        grad_norm_gain,
        gate_share,
        input_share,
        state_share,
        step_share,
        taps_sum[:4],
        taps_sum[4],
        state_sum[:4],
        state_sum[4],
        rest[:heads],
        rest[heads : 2 * heads],
        rest[2 * heads : 3 * heads],
        rest[3 * heads :],
        out_share,
    )


def solution(mesh):
    in_specs = (
        P("dp", "seq", None),
        P("dp", "seq", None),
        P("dp", "seq"),
        P(),
        P("seq", "head"),
        P("seq", "head"),
        P("seq", None),
        P("seq", "head"),
        P(None, "head"),
        P("head"),
        P(),
        P(),
        P("head"),
        P("head"),
        P("head"),
        P("head"),
        P("head", "seq"),
    )
    out_specs = (
        P("dp", "seq", None),
        P("dp", "seq", None),
        P(),
        P("seq", "head"),
        P("seq", "head"),
        P("seq", None),
        P("seq", "head"),
        P(None, "head"),
        P("head"),
        P(),
        P(),
        P("head"),
        P("head"),
        P("head"),
        P("head"),
        P("head", "seq"),
    )
    return jax.shard_map(
        per_device, mesh=mesh, in_specs=in_specs, out_specs=out_specs, check_vma=False
    )
```
